256 devices in a mesh: dp: 4 (over x), expert: 64 (over z, y, core).
Axes of the slice: x: 4, y: 4, z: 8, core: 2. Of those that a mesh axis runs over, the one named last changes fastest.
Arguments:
- rollout_states: bfloat16 [64, 32, 2, 4096], P('expert', 'dp'), may hold values from -30 to 30
- lengths: int32 [32], P('dp'), may hold values from 8 to 128
- group_ids: int32 [32], P('dp'), may hold values from 0 to 3, as said below
- route_ids: int32 [64, 32, 2, 8], P('expert', 'dp'), may hold values from 0 to 63, all different within a row; in each aligned block of 16 rows (0 to 15, 16 to 31, ..., all dimensions but the last counted through in order) at most 4 rows name the same one
- route_weights: float32 [64, 32, 2, 8], P('expert', 'dp'), may hold values from 0.05 to 0.4
- gain_in: float32 [4096], replicated, may hold values from 0.5 to 1.5
- w_gate: bfloat16 [64, 4096, 1024], P('expert', None, 'dp'), may hold values from -0.09375 to 0.09375
- w_up: bfloat16 [64, 4096, 1024], P('expert', None, 'dp'), may hold values from -0.09375 to 0.09375
- w_down: bfloat16 [64, 1024, 4096], P('expert', 'dp'), may hold values from -0.1875 to 0.1875
- gain_out: float32 [4096], replicated, may hold values from 0.5 to 1.5
- head_weight: bfloat16 [4096, 65536], P(None, 'expert'), may hold values from -16 to 16
- targets: int32 [64, 32, 2], P('expert', 'dp'), may hold values from 0 to 65535
- policy_logp: float32 [64, 32, 2], P('expert', 'dp'), may hold values from -14 to -6
Outputs:
- token_kl: float32 [64, 32, 2], P('expert', 'dp')
- row_kl: float32 [32], P('dp')
The draws below stay inside these ranges and needn't reach their ends.
Inputs may be any that keep to these rules, and one draw needn't show every extreme that they name: `group_ids`: every prompt group has exactly 8 rows; group g is owned by index g mod 4 of dp, so every index owns exactly 8 rows. `route_ids`: every token names 8 different experts. Among the 16 tokens of one device no expert is named more than 4 times, and that bound is reached in every draw.
All inputs are finite; a program needn't handle non-finite values.
Results may differ from the reference program's by a relative error of at most 0.0055.
Values may be sent and summed in bfloat16 or wider, within the bound.
No kernel may reach another device: no remote copies, remote signals or barrier semaphores. Data moves between devices by JAX's collectives and lax.ppermute only.
A program may use at most 192 MiB of HBM per device.

```python
import math
import jax
import jax.numpy as jnp
import numpy as np
from jax import lax

D = 4096
FF = 1024
VOCAB = 65536
TOPK = 8
ROW = 128
GSIZE = 8
RPD = 8
OWNERS = 4
SPLITS = 64
EXPERTS = 64
POS = 2
ROWS_ALL = 32
TB = 16
MOST = 4


def shared_direction(key):
    raw_values = jax.random.normal(jax.random.fold_in(key, 7001), (D,), jnp.float32)
    return raw_values / jnp.sqrt(jnp.mean(raw_values * raw_values))


def draw_rollout_states(key, part):
    full_shape = (SPLITS, ROWS_ALL, POS, D)
    state_key = jax.random.fold_in(key, 11)
    value_key = jax.random.fold_in(state_key, 1)
    pick_key = jax.random.fold_in(state_key, 2)
    sign_key = jax.random.fold_in(state_key, 3)
    values = jax.random.normal(value_key, full_shape, jnp.float32)
    chosen = jax.random.randint(pick_key, (SPLITS, ROWS_ALL, POS, 1), 0, 16) == 0
    signs = 2.0 * jax.random.randint(sign_key, (SPLITS, ROWS_ALL, POS, 1), 0, 2).astype(jnp.float32) - 1.0
    direction = shared_direction(key)
    values = jnp.where(chosen, 5.0 * signs * direction + 0.3 * values, values)
    return jnp.clip(values, -30.0, 30.0).astype(jnp.bfloat16)


def draw_head_weight(key, part):
    head_key = jax.random.fold_in(key, 23)
    values = jax.random.normal(head_key, (D, VOCAB), jnp.float32) / math.sqrt(D)
    common = 150.0 * shared_direction(key) / D
    values = values + common[:, None]
    return jnp.clip(values, -16.0, 16.0).astype(jnp.bfloat16)


def draw_group_ids(key, part):
    group_key = jax.random.fold_in(key, 37)
    shuffled = jax.random.permutation(group_key, ROWS_ALL).astype(jnp.int32)
    owners = (shuffled // RPD).astype(jnp.int32)
    member = (owners[:, None] == jnp.arange(OWNERS, dtype=jnp.int32)[None, :]).astype(jnp.int32)
    earlier = jnp.sum((jnp.cumsum(member, axis=0) - member) * member, axis=1)
    return (owners + OWNERS * (earlier // GSIZE)).astype(jnp.int32)


def draw_policy_logp(key, part):
    logp_key = jax.random.fold_in(key, 53)
    center = -math.log(VOCAB)
    spread = jax.random.uniform(logp_key, (SPLITS, ROWS_ALL, POS), jnp.float32, -1.5, 1.5)
    return jnp.clip(center + spread, -14.0, -6.0).astype(jnp.float32)


def plant(array, stream_key, least, high):
    longest = array.shape.index(max(array.shape))
    spots = []
    for shift in (0, 1):
        where = [jax.random.randint(jax.random.fold_in(stream_key, axis), (), 0, length) for axis, length in enumerate(array.shape)]
        where[longest] = (where[longest] + shift) % array.shape[longest]
        spots.append(tuple(where))
    return array.at[spots[0]].set(least).at[spots[1]].set(high)


def block_levels(rng, extent, shards, low, top_value):
    factor_of, own = 1.0, jax.random.fold_in(rng, 6)
    for axis_at, blocks in shards:
        steps = jnp.exp(jax.random.uniform(jax.random.fold_in(own, axis_at), (blocks,), jnp.float32, low / len(shards), top_value / len(shards)))
        factor_of = factor_of * jnp.repeat(steps, extent[axis_at] // blocks).reshape([-1 if axis == axis_at else 1 for axis in range(len(extent))])
    return factor_of


def rank_table(number_of, slope):
    weights = [(1 << 20) // math.isqrt(standing ** slope) + 1 for standing in range(1, number_of + 1)]
    deviation = 1 + sum(weights) // (1 << 30)
    return np.cumsum(np.array([max(1, weight // deviation) for weight in weights]))


def skewed_ids(stream_key, shape, count, lean):
    table = rank_table(count, lean)
    lot = jax.random.randint(jax.random.fold_in(stream_key, 1), shape, 0, int(table[count - 1]))
    rank = jnp.searchsorted(jnp.asarray(table, jnp.int32), lot, side="right")
    return jax.random.permutation(jax.random.fold_in(stream_key, 2), count)[rank].astype(jnp.int32)


def shared_out(stream_key, own, number, rows, count, top, most, slope):
    sequence = jax.random.permutation(stream_key, count)
    heavy_load, usual = portions_of(count, rows * top, most, slope, True), portions_of(count, rows * top, most, slope, False)
    places = jnp.arange(count)

    def named(sizes, offset_by):
        used = int((sizes > 0).sum())
        fixed = max(1, used // 4)
        moved = fixed + (places - fixed + offset_by * (used - fixed)) % max(1, count - fixed)
        return jnp.zeros((count,), jnp.int32).at[sequence[jnp.where(places < fixed, places, moved)]].set(jnp.asarray(sizes, jnp.int32))

    sizes = jnp.where(number % 4 == 0, named(heavy_load, number // 4), named(usual, number - number // 4 - 1))
    mixed = jax.random.permutation(jax.random.fold_in(own, 3), count)
    source_of, receiver = mixed[0:count // 2 * 2:2], mixed[1:count // 2 * 2:2]
    room = jnp.minimum(sizes[source_of] - 1, most - sizes[receiver]) // 2
    room = jnp.where((source_of == sequence[0]) | (receiver == sequence[0]) | (sizes[receiver] == 0), 0, jnp.maximum(room, 0))
    moved = jax.random.randint(jax.random.fold_in(own, 4), (count // 2,), 0, 1 << 20) % (room + 1)
    sizes = sizes.at[source_of].add(-moved).at[receiver].add(moved)
    members = jnp.searchsorted(jnp.cumsum(sizes), jnp.arange(rows * top), side="right").astype(jnp.int32)
    grid = members.reshape(top, rows).T
    grid = grid[jax.random.permutation(jax.random.fold_in(own, 1), rows)]
    offset_by = jax.random.randint(jax.random.fold_in(own, 2), (rows, 1), 0, top)
    return jnp.take_along_axis(grid, (jnp.arange(top)[None, :] + offset_by) % top, axis=1)


def portions_of(number_of, total, bound, slope, full):
    portions = [(1 << 20) // math.isqrt(rank ** slope) + 1 for rank in range(1, number_of + 1)]
    largest = bound if full else min(bound, max(-(-total // number_of), total * portions[0] // sum(portions)))
    least = 1 if total - largest >= number_of - 1 else 0
    counts, spare = [largest] + [least] * (number_of - 1), total - largest - least * (number_of - 1)
    while spare > 0:
        free = [i for i in range(1, number_of) if counts[i] < largest] or [i for i in range(1, number_of) if counts[i] < bound]
        whole, budget = sum([portions[i] for i in free]), spare
        for i in free:
            extra = min(bound - counts[i], max(1, budget * portions[i] // whole), spare)
            counts[i] = counts[i] + extra
            spare = spare - extra
    return np.array(counts)


def noise(key, extent, scale, most, pieces=(), held_as=jnp.bfloat16):
    gain = block_levels(key, extent, pieces, -0.22, 0.18) if pieces else 1.0
    result = jax.random.normal(key, extent, jnp.float32) * scale * gain
    return jnp.minimum(jnp.maximum(result, -most), most).astype(held_as)


def setup_inputs(seed: int = 0) -> dict:
    splits = jax.random.split(jax.random.key(seed), 14)
    rollout_states = draw_rollout_states(jax.random.fold_in(splits[13], 71), 0)
    lengths = plant(jax.random.randint(splits[1], (ROWS_ALL,), 8, ROW + 1), jax.random.fold_in(splits[1], 1), 8, ROW).astype(jnp.int32)
    group_ids = draw_group_ids(jax.random.fold_in(splits[13], 71), 0)
    route_ids_keys = jax.random.split(jax.random.fold_in(splits[3], 1), SPLITS * ROWS_ALL * POS // TB)
    route_ids_turns = jax.random.permutation(jax.random.fold_in(splits[3], 3), SPLITS * ROWS_ALL * POS // TB)
    route_ids = jax.vmap(lambda own, number: shared_out(jax.random.fold_in(splits[3], 2), own, number, TB, EXPERTS, TOPK, MOST, 2))(route_ids_keys, route_ids_turns).reshape((SPLITS, ROWS_ALL, POS, TOPK))
    route_weights = jnp.clip(0.05 + 0.35 * jax.random.uniform(splits[4], (SPLITS, ROWS_ALL, POS, TOPK), jnp.float32) ** block_levels(splits[4], (SPLITS, ROWS_ALL, POS, TOPK), ((0, 64), (1, 4)), -0.2, 0.2), 0.05, 0.4)
    gain_in = jnp.clip(1.0 + 0.1 * jax.random.normal(splits[5], (D,), jnp.float32), 0.5, 1.5)
    w_gate = noise(splits[6], (EXPERTS, D, FF), D ** -0.5, 0.09375, ((0, 64), (2, 4)))
    w_up = noise(splits[7], (EXPERTS, D, FF), D ** -0.5, 0.09375, ((0, 64), (2, 4)))
    w_down = noise(splits[8], (EXPERTS, FF, D), FF ** -0.5, 0.1875, ((0, 64), (1, 4)))
    gain_out = jnp.clip(1.0 + 0.1 * jax.random.normal(splits[9], (D,), jnp.float32), 0.5, 1.5)
    head_weight = draw_head_weight(jax.random.fold_in(splits[13], 71), 0)
    targets = plant(skewed_ids(splits[11], (SPLITS, ROWS_ALL, POS), VOCAB, 2), jax.random.fold_in(splits[11], 3), 0, VOCAB - 1).astype(jnp.int32)
    policy_logp = draw_policy_logp(jax.random.fold_in(splits[13], 71), 0)
    return dict(rollout_states=rollout_states, lengths=lengths, group_ids=group_ids, route_ids=route_ids, route_weights=route_weights, gain_in=gain_in, w_gate=w_gate, w_up=w_up, w_down=w_down, gain_out=gain_out, head_weight=head_weight, targets=targets, policy_logp=policy_logp)


def scaled_norm(values, gain_vec):
    mean_square = lax.optimization_barrier(jnp.mean(values * values, axis=-1, keepdims=True))
    return values * lax.rsqrt(mean_square + 1e-06) * gain_vec

def reference(rollout_states, lengths, group_ids, route_ids, route_weights, gain_in, w_gate, w_up, w_down, gain_out, head_weight, targets, policy_logp):
    owner_index = group_ids % OWNERS
    member = (owner_index[:, None] == jnp.arange(OWNERS, dtype=jnp.int32)[None, :]).astype(jnp.int32)
    owner_slot = lax.optimization_barrier(jnp.sum((jnp.cumsum(member, axis=0) - member) * member, axis=1))
    target_row = (owner_index * RPD + owner_slot).astype(jnp.int32)
    owned_states = jnp.zeros_like(rollout_states).at[:, target_row].set(rollout_states)
    owned_lengths = jnp.zeros_like(lengths).at[target_row].set(lengths)
    features = rollout_states.shape[-1]
    states_flat = owned_states.reshape(-1, features).astype(jnp.float32)
    normed_in = scaled_norm(states_flat, gain_in).astype(jnp.bfloat16)
    expert_ids = route_ids.reshape(-1, TOPK)
    gate_values = route_weights.reshape(-1, TOPK)
    token_count = states_flat.shape[0]
    capacity = OWNERS * SPLITS * MOST
    token_index = jnp.arange(token_count, dtype=jnp.int32)

    def one_expert(running, expert):
        chosen = expert_ids == expert
        is_taken = jnp.any(chosen, axis=1)
        weight = lax.optimization_barrier(jnp.sum(jnp.where(chosen, gate_values, 0.0), axis=1))
        place_at = jnp.cumsum(is_taken.astype(jnp.int32)) - 1
        place_at = jnp.where(is_taken, place_at, capacity).astype(jnp.int32)
        source_rows = jnp.zeros((capacity,), jnp.int32).at[place_at].set(token_index, mode='drop')
        picked = normed_in[source_rows]
        gate_act = jnp.dot(picked, w_gate[expert], preferred_element_type=jnp.float32)
        up_act = jnp.dot(picked, w_up[expert], preferred_element_type=jnp.float32)
        hidden = (jax.nn.silu(gate_act) * up_act).astype(jnp.bfloat16)
        output = jnp.dot(hidden, w_down[expert], preferred_element_type=jnp.float32).astype(jnp.bfloat16)
        back_rows = output[jnp.minimum(place_at, capacity - 1)].astype(jnp.float32)
        return (running + jnp.where(is_taken[:, None], weight[:, None] * back_rows, 0.0), None)
    routed, unused = lax.scan(one_expert, jnp.zeros((token_count, features), jnp.float32), jnp.arange(EXPERTS, dtype=jnp.int32))
    mixed_sum = states_flat + routed
    normed_out = scaled_norm(mixed_sum, gain_out).astype(jnp.bfloat16)
    flat_targets = targets.reshape(-1)

    def block_logp(inputs):
        block_rows, block_targets = inputs
        logits = jnp.dot(block_rows, head_weight, preferred_element_type=jnp.float32)
        peak_value = lax.optimization_barrier(jnp.max(logits, axis=1, keepdims=True))
        shifted = jnp.log(lax.optimization_barrier(jnp.sum(jnp.exp(logits - peak_value), axis=1))) + peak_value[:, 0]
        picked = jnp.take_along_axis(logits, block_targets[:, None], axis=1)[:, 0]
        return picked - shifted
    ref_logp = lax.map(block_logp, (normed_out.reshape(-1, ROW, features), flat_targets.reshape(-1, ROW))).reshape(-1)
    log_ratio = jnp.clip(ref_logp - policy_logp.reshape(-1), -10.0, 10.0)
    token_value = jnp.exp(log_ratio) - log_ratio - 1.0
    position = jnp.arange(SPLITS, dtype=jnp.int32)[:, None, None] * POS + jnp.arange(POS, dtype=jnp.int32)[None, None, :]
    inside = position < owned_lengths[None, :, None]
    token_kl = jnp.where(inside, token_value.reshape(SPLITS, ROWS_ALL, POS), 0.0)
    row_kl = lax.optimization_barrier(jnp.sum(token_kl, axis=(0, 2))) / owned_lengths.astype(jnp.float32)
    return (token_kl, row_kl)
```

```python
import jax
import jax.numpy as jnp
from jax import lax
from jax.sharding import PartitionSpec as P

BF = jnp.bfloat16
F32 = jnp.float32
DP, NZ, NY, NC = 4, 8, 4, 2
EX = NZ * NY * NC
SLOT = 4


def expert_at(z, y, c):
    return ((z % NZ) * NY + y % NY) * NC + c


def places():
    return [(z, y, c) for z in range(NZ) for y in range(NY) for c in range(NC)]


def shifted(dz, dy):
    return [(expert_at(z, y, c), expert_at(z + dz, y + dy, c)) for z, y, c in places()]


def other_core():
    return [(expert_at(z, y, c), expert_at(z, y, 1 - c)) for z, y, c in places()]


def paired(parity):
    out = []
    for x in range(DP):
        for e in range(EX):
            if (e % NC + parity) % 2 == 0:
                peer = x ^ 1
            else:
                peer = (x + 1) % DP if x % 2 else (x - 1) % DP
            out.append((x * EX + e, peer * EX + e))
    return out


def pair_swap(value, parity):
    return lax.ppermute(value, ("dp", "expert"), paired(parity))


def move(value, dz, dy):
    return lax.ppermute(value, "expert", shifted(dz, dy))


def sent_to_all(value, axis):
    copies = jnp.broadcast_to(value, (lax.axis_size(axis), *value.shape))
    return lax.all_to_all(copies, axis, split_axis=0, concat_axis=0, tiled=True)


def plane_groups():
    return [[expert_at(z, y, c) for y in range(NY) for c in range(NC)] for z in range(NZ)]


def column_groups():
    return [[expert_at(z, y, c) for z in range(NZ)] for y in range(NY) for c in range(NC)]


def scaled_norm(values, gain_vec):
    mean_square = jnp.mean(values * values, axis=-1, keepdims=True)
    return values * lax.rsqrt(mean_square + 1e-06) * gain_vec


def dot(a, b):
    return jnp.dot(a, b, preferred_element_type=F32)


def expert_part(rows, weights):
    total = 0.0
    for gate, up, down in weights:
        hidden = (jax.nn.silu(dot(rows, gate)) * dot(rows, up)).astype(BF)
        total = total + dot(hidden, down)
    return total


def gathered_rows(rows):
    first, second = rows[:8], rows[8:]
    up, down = [first], [first]
    for _ in range(4):
        up.append(move(up[-1], 1, 0))
    for _ in range(3):
        down.append(move(down[-1], -1, 0))
    right = move(second, 0, 1)
    left = move(second, 0, -1)
    far = move(right, 0, 1)
    col = jnp.concatenate([second, right, left, far], axis=0)
    col_dy = [0, 1, 3, 2]
    ring = jnp.concatenate([up[0], up[1], up[2], up[3], up[4], down[3], down[2], down[1]], axis=0)
    out = []
    ring_dz = list(range(8))
    r1 = move(ring, 0, 1)
    l1 = move(ring, 0, -1)
    r2 = move(r1[:32], 0, 1)
    l2 = move(l1[32:], 0, -1)
    u, d = [col], [col]
    for _ in range(3):
        u.append(move(u[-1], 1, 0))
        d.append(move(d[-1], -1, 0))
    u4 = move(u[3][:16], 1, 0)
    d4 = move(d[3][16:], -1, 0)
    for dy, piece in ((0, ring), (1, r1), (3, l1)):
        out.append(([(dz, dy, 0) for dz in ring_dz], piece))
    out.append(([(dz, 2, 0) for dz in ring_dz[:4]], r2))
    out.append(([(dz, 2, 0) for dz in ring_dz[4:]], l2))
    for dz, piece in ((0, u[0]), (1, u[1]), (2, u[2]), (3, u[3]), (7, d[1]), (6, d[2]), (5, d[3])):
        out.append(([(dz, dy, 1) for dy in col_dy], piece))
    out.append(([(4, dy, 1) for dy in col_dy[:2]], u4))
    out.append(([(4, dy, 1) for dy in col_dy[2:]], d4))
    order, pieces = [], []
    for names, piece in out:
        order += names
        pieces.append(piece)
    return order, jnp.concatenate(pieces, axis=0)


def on_device(
    rollout_states,
    lengths,
    group_ids,
    route_ids,
    route_weights,
    gain_in,
    w_gate,
    w_up,
    w_down,
    gain_out,
    head_weight,
    targets,
    policy_logp,
):
    own_owner = lax.axis_index("dp")
    own_expert = lax.axis_index("expert")
    rows, pos_count, features = rollout_states.shape[1:]
    tokens = rows * pos_count
    meta = sent_to_all(jnp.stack([group_ids, lengths]), "dp")
    all_states = sent_to_all(rollout_states[0], "dp").reshape(DP * rows, pos_count * features)
    all_owner = meta[:, 0].reshape(-1) % DP
    all_lengths = meta[:, 1].reshape(-1)
    same = all_owner[None, :] == all_owner[:, None]
    ids = jnp.arange(DP * rows, dtype=jnp.int32)
    rank = jnp.sum((same & (ids[None, :] < ids[:, None])).astype(jnp.int32), axis=1)
    place = jnp.where(all_owner == own_owner, rank, rows)
    pick = place[None, :] == jnp.arange(rows, dtype=jnp.int32)[:, None]
    owned_lengths = jnp.sum(jnp.where(pick, all_lengths[None, :], 0), axis=1)
    states_wide = dot(pick.astype(BF), all_states).reshape(tokens, features)
    all_states, w_gate, w_up, w_down = lax.optimization_barrier((all_states, w_gate, w_up, w_down))
    mine = (w_gate[0], w_up[0], w_down[0])
    theirs = tuple(pair_swap(w, 0) for w in mine)
    normed_in = scaled_norm(states_wide, gain_in).astype(BF)
    expert_ids = route_ids.reshape(tokens, -1)
    gates = route_weights.reshape(tokens, -1)
    named = expert_ids[:, :, None] == jnp.arange(EX, dtype=jnp.int32)
    member = jnp.any(named, axis=1)
    weight = jnp.sum(jnp.where(named, gates[:, :, None], 0.0), axis=1)
    earlier = jnp.tril(jnp.ones((tokens, tokens), F32), -1)
    slot = dot(earlier, member.astype(F32)).astype(jnp.int32)
    holds = member[:, :, None] & (slot[:, :, None] == jnp.arange(SLOT, dtype=jnp.int32))
    spread = holds.reshape(tokens, EX * SLOT)
    sender = lax.dot_general(
        spread.astype(BF), normed_in, (((0,), (0,)), ((), ())), preferred_element_type=F32
    ).astype(BF)
    arrived = lax.all_to_all(
        sender.reshape(EX, SLOT, features), "expert", split_axis=0, concat_axis=0, tiled=True
    ).reshape(EX * SLOT, features)
    paired_rows = pair_swap(arrived, 1)
    both = (mine, theirs)
    for_pair = expert_part(paired_rows, both).astype(BF)
    from_pair = pair_swap(for_pair, 1)
    worked = (expert_part(arrived, both) + from_pair.astype(F32)).astype(BF)
    returned = lax.all_to_all(
        worked.reshape(EX, SLOT, features), "expert", split_axis=0, concat_axis=0, tiled=True
    ).reshape(EX * SLOT, features)
    wide = jnp.where(holds, weight[:, :, None], 0.0).reshape(tokens, EX * SLOT)
    parts, rest = [], wide
    for _ in range(3):
        part = lax.reduce_precision(rest, 8, 7)
        parts.append(part.astype(BF))
        rest = rest - part
    routed = dot(jnp.concatenate(parts, axis=0), returned)
    routed = routed[:tokens] + routed[tokens : 2 * tokens] + routed[2 * tokens :]
    mixed_sum = states_wide + routed
    final_rows = scaled_norm(mixed_sum, gain_out).astype(BF)
    order, same_core = gathered_rows(final_rows)
    cross_core = lax.ppermute(same_core, "expert", other_core())
    vocab_part = head_weight.shape[1]
    vocab_start = own_expert * vocab_part
    flat_targets = targets.reshape(-1)
    all_targets = sent_to_all(flat_targets, "expert")
    own_z, own_y, own_c = own_expert // (NY * NC), (own_expert // NC) % NY, own_expert % NC
    dz = jnp.array([o[0] for o in order], jnp.int32)
    dy = jnp.array([o[1] for o in order], jnp.int32)
    half = jnp.array([o[2] for o in order], jnp.int32)
    from_z, from_y = (own_z - dz) % NZ, (own_y - dy) % NY
    column = vocab_start + jnp.arange(vocab_part, dtype=jnp.int32)
    stats = []
    for flip, block in ((0, same_core), (1, cross_core)):
        core = (own_c + flip) % 2
        source = (from_z * NY + from_y) * NC + core
        where_at = source * 2 + half
        perm = where_at[:, None] == jnp.arange(EX * 2, dtype=jnp.int32)[None, :]
        target = jnp.sum(
            jnp.where(perm[:, :, None], all_targets.reshape(1, EX * 2, 8), 0), axis=1
        ).reshape(-1)
        logits = dot(block, head_weight)
        peak = jnp.max(logits, axis=1)
        mass = jnp.sum(jnp.exp(logits - peak[:, None]), axis=1)
        hit = jnp.sum(jnp.where(column[None, :] == target[:, None], logits, 0.0), axis=1)
        three = jnp.stack([peak, mass, hit]).reshape(3, len(order), 8)
        stats.append(jnp.sum(jnp.where(perm[None, :, :, None], three[:, :, None, :], 0.0), axis=1))
    stats = stats[0] + stats[1]
    stats = stats.reshape(3, EX, tokens).transpose(1, 0, 2)
    back = lax.all_to_all(stats, "expert", split_axis=0, concat_axis=0, tiled=True)
    peaks, masses, hits = back[:, 0], back[:, 1], back[:, 2]
    peak_mine = jnp.max(peaks, axis=0)
    mass_mine = jnp.sum(masses * jnp.exp(peaks - peak_mine[None, :]), axis=0)
    ref_logp = jnp.sum(hits, axis=0) - (peak_mine + jnp.log(mass_mine))
    log_ratio = jnp.clip(ref_logp - policy_logp.reshape(-1), -10.0, 10.0)
    token_value = jnp.exp(log_ratio) - log_ratio - 1.0
    position = own_expert * pos_count + jnp.arange(pos_count, dtype=jnp.int32)
    inside = position[None, :] < owned_lengths[:, None]
    token_kl = jnp.where(inside, token_value.reshape(rows, pos_count), 0.0)
    row_total = sent_to_all(jnp.sum(token_kl, axis=1), "expert").sum(axis=0)
    row_kl = row_total / owned_lengths.astype(F32)
    return (token_kl.reshape(1, rows, pos_count), row_kl)


def solution(mesh):
    in_specs = (
        P("expert", "dp", None, None),
        P("dp"),
        P("dp"),
        P("expert", "dp", None, None),
        P("expert", "dp", None, None),
        P(),
        P("expert", None, "dp"),
        P("expert", None, "dp"),
        P("expert", "dp", None),
        P(),
        P(None, "expert"),
        P("expert", "dp", None),
        P("expert", "dp", None),
    )
    out_specs = (P("expert", "dp", None), P("dp"))
    return jax.shard_map(
        on_device, mesh=mesh, in_specs=in_specs, out_specs=out_specs, check_vma=False
    )
```

```python
import jax
import jax.numpy as jnp
import numpy as np
from jax import lax
from jax.experimental import pallas as pl
from jax.experimental.pallas import tpu as pltpu
from jax.sharding import Mesh
from jax.sharding import PartitionSpec as P

BF = jnp.bfloat16
F32 = jnp.float32
I32 = jnp.int32
NX, NZ, NY, NC = 4, 8, 4, 2
PLANE = NY * NC
SLOT = 4
EXPERT = ("z", "y", "c")


def shift(value, axis, by):
    size = {"dp": NX, "z": NZ, "y": NY, "c": NC}[axis]
    return lax.ppermute(value, axis, [(i, (i + by) % size) for i in range(size)])


def pair_swap(value, parity):
    perm = []
    for x in range(NX):
        for e in range(NZ * NY * NC):
            if (e % NC + parity) % 2 == 0:
                peer = x ^ 1
            else:
                peer = (x + 1) % NX if x % 2 else (x - 1) % NX
            perm.append((x * NZ * PLANE + e, peer * NZ * PLANE + e))
    return lax.ppermute(value, ("dp", *EXPERT), perm)


def sent_to_all(value, axis):
    copies = jnp.broadcast_to(value, (lax.axis_size(axis), *value.shape))
    return lax.all_to_all(copies, axis, split_axis=0, concat_axis=0, tiled=True)


def turned(value, own, size):
    at = jnp.arange(size, dtype=I32)
    one = (own - at[:, None]) % size == at[None, :]
    one = one.reshape(size, size, *([1] * (value.ndim - 1)))
    return jnp.sum(jnp.where(one, value[None], jnp.zeros((), value.dtype)), axis=1)


def scaled_norm(values, gain_vec):
    mean_square = jnp.mean(values * values, axis=-1, keepdims=True)
    return values * lax.rsqrt(mean_square + 1e-06) * gain_vec


def dot(a, b):
    return jnp.dot(a, b, preferred_element_type=F32)


def three_parts(value):
    parts = []
    for _ in range(3):
        part = lax.reduce_precision(value, 8, 7)
        parts.append(part)
        value = value - part
    return parts


def expert_kernel(*refs, adds):
    rows, weights, rest = refs[0], refs[1:7], refs[7:]
    extra = rest[0] if adds else None
    out, gate, up, down, sems = rest[adds:]
    buffers = (gate, up, down)
    order = [(0, 0), (1, 0), (0, 1), (1, 1), (2, 0), (2, 1)]
    copies = {}
    for kind, side in order:
        copies[kind, side] = pltpu.make_async_copy(
            weights[side * 3 + kind], buffers[kind].at[side], sems.at[side * 3 + kind]
        )
        copies[kind, side].start()
    hidden = []
    for side in range(2):
        copies[0, side].wait()
        gated = dot(rows[...], gate[side])
        copies[1, side].wait()
        hidden.append((gated * jax.nn.sigmoid(gated) * dot(rows[...], up[side])).astype(BF))
    copies[2, 0].wait()
    copies[2, 1].wait()
    step = 512
    for at in range(0, out.shape[1], step):
        cols = slice(at, at + step)
        total = dot(hidden[0], down[0, :, cols]) + dot(hidden[1], down[1, :, cols])
        if adds:
            total = total + extra[:, cols].astype(F32)
        out[:, cols] = total.astype(BF)


def expert_part(rows, mine, theirs, extra=None):
    adds = extra is not None
    features, units = mine[0].shape
    count = rows.shape[0]
    vmem = pl.BlockSpec(memory_space=pltpu.VMEM)
    flops = 12 * count * features * units
    return pl.pallas_call(
        lambda *refs: expert_kernel(*refs, adds=int(adds)),
        out_shape=jax.ShapeDtypeStruct(rows.shape, BF),
        in_specs=[vmem] + [pl.BlockSpec(memory_space=pl.ANY)] * 6 + [vmem] * adds,
        out_specs=vmem,
        scratch_shapes=[
            pltpu.VMEM((2, features, units), BF),
            pltpu.VMEM((2, features, units), BF),
            pltpu.VMEM((2, units, features), BF),
            pltpu.SemaphoreType.DMA((6,)),
        ],
        compiler_params=pltpu.CompilerParams(vmem_limit_bytes=40 * 2**20),
        cost_estimate=pl.CostEstimate(
            flops=flops, bytes_accessed=12 * features * units, transcendentals=2 * count * units
        ),
        name="expert",
    )(rows, *mine, *theirs, *([extra] if adds else []))


def on_device(
    rollout_states,
    lengths,
    group_ids,
    route_ids,
    route_weights,
    gain_in,
    w_gate,
    w_up,
    w_down,
    gain_out,
    head_weight,
    targets,
    policy_logp,
):
    own_x, own_z, own_y, own_c = (lax.axis_index(a) for a in ("dp", "z", "y", "c"))
    rows, pos_count, features = rollout_states.shape[1:]
    tokens = rows * pos_count
    wide = pos_count * features
    facts = jnp.pad(jnp.stack([group_ids, lengths], axis=1).astype(BF), ((0, 0), (0, 126)))
    block = jnp.concatenate([rollout_states.reshape(rows, wide), facts], axis=1)
    blocks = [block, shift(block, "dp", 1), shift(block, "dp", 2), shift(block, "dp", -1)]
    every = jnp.concatenate(blocks, axis=0)
    every, w_gate, w_up, w_down = lax.optimization_barrier((every, w_gate, w_up, w_down))
    local = jnp.arange(rows, dtype=I32)
    ids = jnp.concatenate([((own_x - k) % NX) * rows + local for k in range(NX)])
    owner = every[:, wide].astype(I32) % NX
    before = (owner[None, :] == owner[:, None]) & (ids[None, :] < ids[:, None])
    rank = jnp.sum(before.astype(I32), axis=1)
    place = jnp.where(owner == own_x, rank, rows)
    pick = (place[None, :] == local[:, None]).astype(BF)
    owned = dot(pick, every)
    owned_lengths = owned[:, wide + 1].astype(I32)
    states_wide = owned[:, :wide].reshape(tokens, features)
    mine = (w_gate[0], w_up[0], w_down[0])
    theirs = []
    for part in mine:
        theirs.append(pair_swap(part, 0))
    normed_in = scaled_norm(states_wide, gain_in).astype(BF)
    target = targets.reshape(tokens, 1)
    info = [route_ids.reshape(tokens, -1).astype(F32)]
    info += three_parts(route_weights.reshape(tokens, -1))
    info += three_parts(policy_logp.reshape(tokens, 1))
    info += [(target // 256).astype(F32), (target % 256).astype(F32)]
    info = jnp.concatenate(info, axis=1)
    width = info.shape[1]
    info = jnp.pad(info, ((0, 0), (0, 128 - width))).astype(BF)
    own = jnp.concatenate([normed_in, info], axis=1)
    up, down = [own], [own]
    for step in range(4):
        up.append(shift(up[-1], "z", 1))
        if step < 3:
            down.append(shift(down[-1], "z", -1))
    ring = jnp.concatenate(up + down[:0:-1], axis=0)
    count = NZ * tokens
    facts = ring[:, features:].astype(F32)
    topk = route_ids.shape[-1]
    named_as = facts[:, :topk].astype(I32) - own_z * PLANE
    named = named_as[:, :, None] == jnp.arange(PLANE, dtype=I32)
    member = jnp.any(named, axis=1)
    t = np.arange(count)
    earlier = (t[:, None] // tokens == t[None, :] // tokens) & (t[None, :] < t[:, None])
    rank = dot(jnp.asarray(earlier, BF), member.astype(BF)).astype(I32)
    slot = jnp.where(member, rank + jnp.asarray(t[:, None] // tokens * SLOT, I32), -1)
    holds = slot[:, :, None] == jnp.arange(NZ * SLOT, dtype=I32)
    spread = holds.reshape(count, PLANE * NZ * SLOT)
    sender = lax.dot_general(
        spread.astype(BF),
        ring[:, :features],
        (((0,), (0,)), ((), ())),
        preferred_element_type=F32,
    ).astype(BF)
    arrived = lax.all_to_all(
        sender.reshape(PLANE, NZ * SLOT, features), ("y", "c"), 0, 0, tiled=True
    ).reshape(-1, features)
    paired_rows = pair_swap(arrived, 1)
    column_targets = (facts[:, width - 2] * 256 + facts[:, width - 1]).astype(I32)
    column_targets, arrived = lax.optimization_barrier((column_targets, arrived))
    plane_targets = sent_to_all(column_targets, ("y", "c")).reshape(NY, NC, NZ, tokens)
    for_pair = expert_part(paired_rows, mine, theirs)
    from_pair = pair_swap(for_pair, 1)
    partial_own = expert_part(arrived, mine, theirs)
    worked = (partial_own.astype(F32) + from_pair.astype(F32)).astype(BF)
    returned = lax.all_to_all(
        worked.reshape(PLANE, NZ * SLOT, features), ("y", "c"), 0, 0, tiled=True
    ).reshape(-1, features)
    parts = []
    for k in range(3):
        part = facts[:, topk * (k + 1) : topk * (k + 2)]
        part = jnp.sum(jnp.where(named, part[:, :, None], 0.0), axis=1)
        part = jnp.where(holds, part[:, :, None], 0.0)
        parts.append(part.reshape(count, PLANE * NZ * SLOT).astype(BF))
    partial = sum(dot(part, returned) for part in parts)
    routed = partial[:tokens]
    for k in range(1, NZ):
        sent = partial[k * tokens : (k + 1) * tokens].astype(BF)
        routed = routed + shift(sent, "z", -k).astype(F32)
    mixed_sum = states_wide + routed
    final_rows = scaled_norm(mixed_sum, gain_out).astype(BF)
    right = shift(final_rows, "y", 1)
    left = shift(final_rows, "y", -1)
    far = shift(right, "y", 1)
    col = jnp.concatenate([final_rows, right, far, left], axis=0)
    chunks = [([0], [col])]
    u, d = col, col
    for k in range(1, 4):
        u, d = shift(u, "z", 1), shift(d, "z", -1)
        chunks.append(([k, NZ - k], [u, d]))
    half = u.shape[0] // 2
    chunks.append(([4], [shift(u[:half], "z", 1), shift(d[half:], "z", -1)]))
    vocab_part = head_weight.shape[1]
    own_expert = (own_z * NY + own_y) * NC + own_c
    column = own_expert * vocab_part + jnp.arange(vocab_part, dtype=I32)
    by_dy = turned(plane_targets, own_y, NY)
    by_place = turned(by_dy.transpose(1, 2, 0, 3), own_c, NC)
    found = {}
    for dzs, pieces in chunks:
        other = [shift(piece, "c", 1) for piece in pieces]
        stacked = jnp.concatenate(pieces + other, axis=0)
        wanted = jnp.stack([by_place[dc, dz] for dc in range(NC) for dz in dzs]).reshape(-1)
        logits = dot(stacked, head_weight)
        peak = jnp.max(logits, axis=1)
        mass = jnp.sum(jnp.exp(logits - peak[:, None]), axis=1)
        hit = jnp.sum(jnp.where(column[None, :] == wanted[:, None], logits, 0.0), axis=1)
        three = jnp.stack([peak, mass, hit]).reshape(3, NC, len(dzs), NY, tokens)
        for i, dz in enumerate(dzs):
            found[dz] = three[:, :, i]
    stats = jnp.stack([found[dz] for dz in range(NZ)], axis=3)
    stats = turned(stats.transpose(1, 2, 0, 3, 4), own_c, NC)
    stats = turned(stats.transpose(1, 0, 2, 3, 4), own_y, NY)

    def joined(many):
        peak = jnp.max(many[:, 0], axis=0)
        mass = jnp.sum(many[:, 1] * jnp.exp(many[:, 0] - peak[None]), axis=0)
        return jnp.stack([peak, mass, jnp.sum(many[:, 2], axis=0)])

    stats = stats.reshape(PLANE, 3, NZ * tokens)
    many = lax.all_to_all(stats, ("y", "c"), 0, 0, tiled=True).reshape(PLANE, 3, NZ, tokens)
    by_z = turned(joined(many).transpose(1, 0, 2), own_z, NZ).transpose(1, 0, 2)
    many = sent_to_all(by_z.reshape(3, NZ * tokens), "z").reshape(NZ, 3, NZ, tokens)
    peak, mass, hit = joined(many)
    ref_logp = hit - (peak + jnp.log(mass))
    policy = facts[:, 4 * topk] + facts[:, 4 * topk + 1] + facts[:, 4 * topk + 2]
    policy = turned(policy.reshape(NZ, tokens), own_z, NZ)
    log_ratio = jnp.clip(ref_logp - policy, -10.0, 10.0)
    token_value = (jnp.exp(log_ratio) - log_ratio - 1.0).reshape(NZ, rows, pos_count)
    at_z = jnp.arange(NZ, dtype=I32)
    position = ((at_z * NY + own_y) * NC + own_c)[:, None] * pos_count
    position = position + jnp.arange(pos_count, dtype=I32)[None, :]
    inside = position[:, None, :] < owned_lengths[None, :, None]
    column_kl = jnp.where(inside, token_value, 0.0)
    token_kl = jnp.sum(jnp.where((at_z == own_z)[:, None, None], column_kl, 0.0), axis=0)
    row_total = sent_to_all(jnp.sum(column_kl, axis=(0, 2)), ("y", "c")).sum(axis=0)
    row_kl = row_total / owned_lengths.astype(F32)
    return (token_kl.reshape(1, rows, pos_count), row_kl)


def solution(mesh):
    cut = Mesh(mesh.devices.reshape(NX, NZ, NY, NC), ("dp", *EXPERT))
    in_specs = (
        P(EXPERT, "dp", None, None),
        P("dp"),
        P("dp"),
        P(EXPERT, "dp", None, None),
        P(EXPERT, "dp", None, None),
        P(),
        P(EXPERT, None, "dp"),
        P(EXPERT, None, "dp"),
        P(EXPERT, "dp", None),
        P(),
        P(None, EXPERT),
        P(EXPERT, "dp", None),
        P(EXPERT, "dp", None),
    )
    out_specs = (P(EXPERT, "dp", None), P("dp"))
    return jax.shard_map(on_device, mesh=cut, in_specs=in_specs, out_specs=out_specs, check_vma=False)
```

```python
import jax
import jax.numpy as jnp
import numpy as np
from jax import lax
from jax.experimental import pallas as pl
from jax.experimental.layout import Layout, with_layout_constraint
from jax.experimental.pallas import tpu as pltpu
from jax.sharding import Mesh
from jax.sharding import PartitionSpec as P

BF = jnp.bfloat16
F32 = jnp.float32
I32 = jnp.int32
NX, NZ, NY, NC = 4, 8, 4, 2
PLANE = NY * NC
SLOT = 4
HALVES = ([0, 3, 4, 5], [1, 2, 6, 7])
EXPERT = ("z", "y", "c")


def shift(value, axis, by):
    size = {"dp": NX, "z": NZ, "y": NY, "c": NC}[axis]
    return lax.ppermute(value, axis, [(i, (i + by) % size) for i in range(size)])


def pair_swap(value, parity):
    perm = []
    for x in range(NX):
        for e in range(NZ * NY * NC):
            if (e % NC + parity) % 2 == 0:
                peer = x ^ 1
            else:
                peer = (x + 1) % NX if x % 2 else (x - 1) % NX
            perm.append((x * NZ * PLANE + e, peer * NZ * PLANE + e))
    return lax.ppermute(value, ("dp", *EXPERT), perm)


def sent_to_all(value, axis):
    copies = jnp.broadcast_to(value, (lax.axis_size(axis), *value.shape))
    return lax.all_to_all(copies, axis, split_axis=0, concat_axis=0, tiled=True)


def turned(value, own, size):
    at = jnp.arange(size, dtype=I32)
    one = (own - at[:, None]) % size == at[None, :]
    one = one.reshape(size, size, *([1] * (value.ndim - 1)))
    return jnp.sum(jnp.where(one, value[None], jnp.zeros((), value.dtype)), axis=1)


def scaled_norm(values, gain_vec):
    mean_square = jnp.mean(values * values, axis=-1, keepdims=True)
    return values * lax.rsqrt(mean_square + 1e-06) * gain_vec


def plain(value):
    return with_layout_constraint(value, Layout(tuple(range(value.ndim))))


def dot(a, b):
    return jnp.dot(a, b, preferred_element_type=F32)


def three_parts(value):
    parts = []
    for _ in range(3):
        part = lax.reduce_precision(value, 8, 7)
        parts.append(part)
        value = value - part
    return parts


def expert_kernel(*refs, adds):
    rows, weights, rest = refs[0], refs[1:7], refs[7:]
    extra = rest[0] if adds else None
    out, gate, up, down, sems = rest[adds:]
    buffers = (gate, up, down)
    order = [(0, 0), (1, 0), (0, 1), (1, 1), (2, 0), (2, 1)]
    copies = {}
    for kind, side in order:
        copies[kind, side] = pltpu.make_async_copy(
            weights[side * 3 + kind], buffers[kind].at[side], sems.at[side * 3 + kind]
        )
        copies[kind, side].start()
    hidden = []
    for side in range(2):
        copies[0, side].wait()
        gated = dot(rows[...], gate[side])
        copies[1, side].wait()
        hidden.append((gated * jax.nn.sigmoid(gated) * dot(rows[...], up[side])).astype(BF))
    copies[2, 0].wait()
    copies[2, 1].wait()
    step = 512
    for at in range(0, out.shape[1], step):
        cols = slice(at, at + step)
        total = dot(hidden[0], down[0, :, cols]) + dot(hidden[1], down[1, :, cols])
        if adds:
            total = total + extra[:, cols].astype(F32)
        out[:, cols] = total.astype(BF)


def expert_part(rows, mine, theirs, extra=None):
    adds = extra is not None
    features, units = mine[0].shape
    count = rows.shape[0]
    vmem = pl.BlockSpec(memory_space=pltpu.VMEM)
    flops = 12 * count * features * units
    return pl.pallas_call(
        lambda *refs: expert_kernel(*refs, adds=int(adds)),
        out_shape=jax.ShapeDtypeStruct(rows.shape, BF),
        in_specs=[vmem] + [pl.BlockSpec(memory_space=pl.ANY)] * 6 + [vmem] * adds,
        out_specs=vmem,
        scratch_shapes=[
            pltpu.VMEM((2, features, units), BF),
            pltpu.VMEM((2, features, units), BF),
            pltpu.VMEM((2, units, features), BF),
            pltpu.SemaphoreType.DMA((6,)),
        ],
        compiler_params=pltpu.CompilerParams(vmem_limit_bytes=40 * 2**20),
        cost_estimate=pl.CostEstimate(
            flops=flops, bytes_accessed=12 * features * units, transcendentals=2 * count * units
        ),
        name="expert",
    )(rows, *mine, *theirs, *([extra] if adds else []))


def logits_kernel(*refs, sizes):
    count = len(sizes)
    pieces, wanted, head = refs[:count], refs[count], refs[count + 1]
    out, stacked, weights, logits, row_sems, sems = refs[count + 2 :]
    loads, at = [], 0
    for i, size in enumerate(sizes):
        loads.append(
            pltpu.make_async_copy(pieces[i], stacked.at[pl.ds(at, size)], row_sems.at[i])
        )
        at += size
    parts = sems.shape[0]
    wide = head.shape[1] // parts
    copies = []
    for n in range(parts):
        cols = pl.ds(n * wide, wide)
        copies.append(pltpu.make_async_copy(head.at[:, cols], weights.at[:, cols], sems.at[n]))
    for copy in loads + copies:
        copy.start()
    for load in loads:
        load.wait()
    for n in range(parts):
        copies[n].wait()
        cols = slice(n * wide, (n + 1) * wide)
        logits[:, cols] = dot(stacked[...], weights[:, cols])
    step = 16

    def some_rows(i, carry):
        here = pl.ds(pl.multiple_of(i * step, step), step)
        values = logits[here, :]
        peak = jnp.max(values, axis=1, keepdims=True)
        mass = jnp.sum(jnp.exp(values - peak), axis=1, keepdims=True)
        lane = lax.broadcasted_iota(I32, values.shape, 1)
        hit = jnp.sum(jnp.where(lane == wanted[here, :], values, 0.0), axis=1, keepdims=True)
        slot = lax.broadcasted_iota(I32, (step, 128), 1)
        out[here, :] = jnp.where(slot == 0, peak, jnp.where(slot == 1, mass, hit))
        return carry

    lax.fori_loop(0, at // step, some_rows, 0)


def logits_part(pieces, wanted, head):
    sizes = [piece.shape[0] for piece in pieces]
    count = sum(sizes)
    features, entries = head.shape
    vmem = pl.BlockSpec(memory_space=pltpu.VMEM)
    anywhere = pl.BlockSpec(memory_space=pl.ANY)
    return pl.pallas_call(
        lambda *refs: logits_kernel(*refs, sizes=sizes),
        out_shape=jax.ShapeDtypeStruct((count, 128), F32),
        in_specs=[anywhere] * len(pieces) + [vmem, anywhere],
        out_specs=vmem,
        scratch_shapes=[
            pltpu.VMEM((count, features), BF),
            pltpu.VMEM((features, entries), BF),
            pltpu.VMEM((count, entries), F32),
            pltpu.SemaphoreType.DMA((len(pieces),)),
            pltpu.SemaphoreType.DMA((4,)),
        ],
        compiler_params=pltpu.CompilerParams(vmem_limit_bytes=32 * 2**20),
        cost_estimate=pl.CostEstimate(
            flops=2 * count * features * entries,
            bytes_accessed=2 * features * entries,
            transcendentals=count * entries,
        ),
        name="logits",
    )(*pieces, wanted.reshape(count, 1), head)


def on_device(
    rollout_states,
    lengths,
    group_ids,
    route_ids,
    route_weights,
    gain_in,
    w_gate,
    w_up,
    w_down,
    gain_out,
    head_weight,
    targets,
    policy_logp,
):
    own_x, own_z, own_y, own_c = (lax.axis_index(a) for a in ("dp", "z", "y", "c"))
    rows, pos_count, features = rollout_states.shape[1:]
    tokens = rows * pos_count
    wide = pos_count * features
    facts = jnp.pad(jnp.stack([group_ids, lengths], axis=1).astype(BF), ((0, 0), (0, 126)))
    block = jnp.concatenate([rollout_states.reshape(rows, wide), facts], axis=1)
    blocks = [block, shift(block, "dp", 1), shift(block, "dp", 2), shift(block, "dp", -1)]
    every = jnp.concatenate(blocks, axis=0)
    every, w_gate, w_up, w_down = lax.optimization_barrier((every, w_gate, w_up, w_down))
    local = jnp.arange(rows, dtype=I32)
    ids = jnp.concatenate([((own_x - k) % NX) * rows + local for k in range(NX)])
    owner = every[:, wide].astype(I32) % NX
    before = (owner[None, :] == owner[:, None]) & (ids[None, :] < ids[:, None])
    rank = jnp.sum(before.astype(I32), axis=1)
    place = jnp.where(owner == own_x, rank, rows)
    pick = (place[None, :] == local[:, None]).astype(BF)
    owned = dot(pick, every)
    owned_lengths = owned[:, wide + 1].astype(I32)
    states_wide = owned[:, :wide].reshape(tokens, features)
    mine = (w_gate[0], w_up[0], w_down[0])
    theirs = []
    for part in mine:
        theirs.append(pair_swap(part, 0))
    normed_in = scaled_norm(states_wide, gain_in).astype(BF)
    target = targets.reshape(tokens, 1)
    info = [route_ids.reshape(tokens, -1).astype(F32)]
    info += three_parts(route_weights.reshape(tokens, -1))
    info += three_parts(policy_logp.reshape(tokens, 1))
    info += [(target // 256).astype(F32), (target % 256).astype(F32)]
    info = jnp.concatenate(info, axis=1)
    width = info.shape[1]
    info = jnp.pad(info, ((0, 0), (0, 128 - width))).astype(BF)
    own = jnp.concatenate([normed_in, info], axis=1)
    up, down = [own], [own]
    for step in range(4):
        up.append(shift(up[-1], "z", 1))
        if step < 3:
            down.append(shift(down[-1], "z", -1))
    ring = up + down[:0:-1]
    topk = route_ids.shape[-1]
    halves = []
    for dzs in HALVES:
        rows_in = jnp.concatenate([ring[dz] for dz in dzs], axis=0)
        count = rows_in.shape[0]
        facts = plain(rows_in[:, features:]).astype(F32)
        named = facts[:, :topk].astype(I32) - own_z * PLANE
        named = named[:, :, None] == jnp.arange(PLANE, dtype=I32)
        member = jnp.any(named, axis=1)
        t = np.arange(count)
        earlier = (t[:, None] // tokens == t[None, :] // tokens) & (t[None, :] < t[:, None])
        rank = dot(jnp.asarray(earlier, BF), member.astype(BF)).astype(I32)
        slot = jnp.where(member, rank + jnp.asarray(t[:, None] // tokens * SLOT, I32), -1)
        spots = len(dzs) * SLOT
        at = jnp.arange(spots, dtype=I32)
        spread = (slot.T[:, None, :] == at[None, :, None]).reshape(PLANE * spots, count)
        sender = dot(spread.astype(BF), rows_in[:, :features]).astype(BF)
        holds = slot[:, :, None] == at
        parts = []
        for k in range(3):
            part = facts[:, topk * (k + 1) : topk * (k + 2)]
            part = jnp.sum(jnp.where(named, part[:, :, None], 0.0), axis=1)
            part = jnp.where(holds, part[:, :, None], 0.0)
            parts.append(part.reshape(count, PLANE * spots).astype(BF))
        arrived = lax.all_to_all(
            sender.reshape(PLANE, spots, features), ("y", "c"), 0, 0, tiled=True
        ).reshape(-1, features)
        paired_rows = pair_swap(arrived, 1)
        halves.append((dzs, spots, parts, arrived, paired_rows))
    facts = jnp.concatenate([plain(block[:, features:]) for block in ring], axis=0).astype(F32)
    policy = facts[:, 4 * topk] + facts[:, 4 * topk + 1] + facts[:, 4 * topk + 2]
    column = jnp.stack([facts[:, width - 2] * 256 + facts[:, width - 1], policy])
    column, *_ = lax.optimization_barrier((column, halves[1][3]))
    plane = sent_to_all(column, ("y", "c")).reshape(NY, NC, 2, NZ, tokens)
    plane_targets, plane_policy = plane[:, :, 0].astype(I32), plane[:, :, 1]
    from_pair = []
    for half in halves:
        for_pair = expert_part(half[4], mine, theirs)
        from_pair.append(pair_swap(for_pair, 1))
    own_part = expert_part(jnp.concatenate([half[3] for half in halves]), mine, theirs)
    routed = 0.0
    at = 0
    for index, (dzs, spots, parts, arrived, _) in enumerate(halves):
        own, peer = own_part[at : at + len(arrived)], from_pair[index]
        if index == 0:
            own, plane_targets, plane_policy = lax.optimization_barrier(
                (own, plane_targets, plane_policy)
            )
        else:
            own, peer, worked = lax.optimization_barrier((own, peer, worked))
        at += len(arrived)
        worked = (own.astype(F32) + peer.astype(F32)).astype(BF)
        returned = lax.all_to_all(
            worked.reshape(PLANE, spots, features), ("y", "c"), 0, 0, tiled=True
        ).reshape(-1, features)
        partial = sum(dot(part, returned) for part in parts)
        for i, dz in enumerate(dzs):
            share = partial[i * tokens : (i + 1) * tokens]
            if dz:
                share = shift(share.astype(BF), "z", -dz).astype(F32)
            routed = routed + share
    mixed_sum = states_wide + routed
    final_rows = scaled_norm(mixed_sum, gain_out).astype(BF)
    right = shift(final_rows, "y", 1)
    left = shift(final_rows, "y", -1)
    far = shift(right, "y", 1)
    col = jnp.concatenate([final_rows, right, far, left], axis=0)
    chunks = [([0], [col])]
    u, d = col, col
    for k in range(1, 4):
        u, d = shift(u, "z", 1), shift(d, "z", -1)
        chunks.append(([k, NZ - k], [u, d]))
    half = u.shape[0] // 2
    chunks.append(([4], [shift(u[:half], "z", 1), shift(d[half:], "z", -1)]))
    vocab_part = head_weight.shape[1]
    own_expert = (own_z * NY + own_y) * NC + own_c
    vocab_start = own_expert * vocab_part
    by_dy = turned(plane_targets, own_y, NY)
    by_place = turned(by_dy.transpose(1, 2, 0, 3), own_c, NC)
    found = {}
    for dzs, pieces in chunks:
        other = [shift(piece, "c", 1) for piece in pieces]
        wanted = jnp.stack([by_place[dc, dz] for dc in range(NC) for dz in dzs]).reshape(-1)
        three = logits_part(pieces + other, wanted - vocab_start, head_weight)[:, :3]
        three = three.T.reshape(3, NC, len(dzs), NY, tokens)
        for i, dz in enumerate(dzs):
            found[dz] = three[:, :, i]
    stats = jnp.stack([found[dz] for dz in range(NZ)], axis=3)
    stats = turned(stats.transpose(1, 2, 0, 3, 4), own_c, NC)
    stats = turned(stats.transpose(1, 0, 2, 3, 4), own_y, NY)

    def joined(many):
        peak = jnp.max(many[:, 0], axis=0)
        mass = jnp.sum(many[:, 1] * jnp.exp(many[:, 0] - peak[None]), axis=0)
        return jnp.stack([peak, mass, jnp.sum(many[:, 2], axis=0)])

    stats = stats.transpose(2, 3, 0, 1, 4).reshape(3, -1)
    stats = joined(sent_to_all(stats, ("y", "c"))).reshape(3, NZ, -1)
    stats = turned(stats.transpose(1, 0, 2), own_z, NZ).transpose(1, 0, 2).reshape(3, -1)
    peak, mass, hit = joined(sent_to_all(stats, "z"))
    ref_logp = hit - (peak + jnp.log(mass))
    policy = turned(plane_policy.transpose(2, 0, 1, 3), own_z, NZ).reshape(-1)
    log_ratio = jnp.clip(ref_logp - policy, -10.0, 10.0)
    token_value = (jnp.exp(log_ratio) - log_ratio - 1.0).reshape(-1, rows, pos_count)
    at = jnp.arange(NZ * PLANE, dtype=I32)
    position = at[:, None] * pos_count + jnp.arange(pos_count, dtype=I32)[None, :]
    inside = position[:, None, :] < owned_lengths[None, :, None]
    all_kl = jnp.where(inside, token_value, 0.0)
    token_kl = jnp.sum(jnp.where((at == own_expert)[:, None, None], all_kl, 0.0), axis=0)
    row_kl = jnp.sum(all_kl, axis=(0, 2)) / owned_lengths.astype(F32)
    return (token_kl.reshape(1, rows, pos_count), row_kl)


def solution(mesh):
    cut = Mesh(mesh.devices.reshape(NX, NZ, NY, NC), ("dp", *EXPERT))
    in_specs = (
        P(EXPERT, "dp", None, None),
        P("dp"),
        P("dp"),
        P(EXPERT, "dp", None, None),
        P(EXPERT, "dp", None, None),
        P(),
        P(EXPERT, None, "dp"),
        P(EXPERT, None, "dp"),
        P(EXPERT, "dp", None),
        P(),
        P(None, EXPERT),
        P(EXPERT, "dp", None),
        P(EXPERT, "dp", None),
    )
    out_specs = (P(EXPERT, "dp", None), P("dp"))
    return jax.shard_map(on_device, mesh=cut, in_specs=in_specs, out_specs=out_specs, check_vma=False)
```

```python
import jax
import jax.numpy as jnp
import numpy as np
from jax import lax
from jax.experimental import pallas as pl
from jax.experimental.layout import Layout, with_layout_constraint
from jax.experimental.pallas import tpu as pltpu
from jax.sharding import Mesh
from jax.sharding import PartitionSpec as P

BF = jnp.bfloat16
F32 = jnp.float32
I32 = jnp.int32
NX, NZ, NY, NC = 4, 8, 4, 2
PLANE = NY * NC
SLOT = 4
HALVES = ([0, 3, 4, 5], [1, 2, 6, 7])
EXPERT = ("z", "y", "c")


def shift(value, axis, by):
    size = {"dp": NX, "z": NZ, "y": NY, "c": NC}[axis]
    return lax.ppermute(value, axis, [(i, (i + by) % size) for i in range(size)])


def pair_swap(value, parity):
    perm = []
    for x in range(NX):
        for e in range(NZ * NY * NC):
            if (e % NC + parity) % 2 == 0:
                peer = x ^ 1
            else:
                peer = (x + 1) % NX if x % 2 else (x - 1) % NX
            perm.append((x * NZ * PLANE + e, peer * NZ * PLANE + e))
    return lax.ppermute(value, ("dp", *EXPERT), perm)


def sent_to_all(value, axis):
    copies = jnp.broadcast_to(value, (lax.axis_size(axis), *value.shape))
    return lax.all_to_all(copies, axis, split_axis=0, concat_axis=0, tiled=True)


def turned(value, own, size):
    at = jnp.arange(size, dtype=I32)
    one = (own - at[:, None]) % size == at[None, :]
    one = one.reshape(size, size, *([1] * (value.ndim - 1)))
    return jnp.sum(jnp.where(one, value[None], jnp.zeros((), value.dtype)), axis=1)


def scaled_norm(values, gain_vec):
    mean_square = jnp.mean(values * values, axis=-1, keepdims=True)
    return values * lax.rsqrt(mean_square + 1e-06) * gain_vec


def plain(value):
    return with_layout_constraint(value, Layout(tuple(range(value.ndim))))


def dot(a, b):
    return jnp.dot(a, b, preferred_element_type=F32)


def three_parts(value):
    parts = []
    for _ in range(3):
        part = lax.reduce_precision(value, 8, 7)
        parts.append(part)
        value = value - part
    return parts


def expert_kernel(rows, gate_0, up_0, down_0, gate_1, up_1, down_1, out):
    hidden = []
    for gate, up in ((gate_0, up_0), (gate_1, up_1)):
        gated = dot(rows[...], gate[...])
        hidden.append((gated * jax.nn.sigmoid(gated) * dot(rows[...], up[...])).astype(BF))
    step = 1024
    for at in range(0, out.shape[1], step):
        cols = slice(at, at + step)
        total = dot(hidden[0], down_0[:, cols]) + dot(hidden[1], down_1[:, cols])
        out[:, cols] = total


def expert_part(rows, mine, theirs):
    features, units = mine[0].shape
    count = rows.shape[0]
    vmem = pl.BlockSpec(memory_space=pltpu.VMEM)
    return pl.pallas_call(
        expert_kernel,
        out_shape=jax.ShapeDtypeStruct(rows.shape, F32),
        in_specs=[vmem] * 7,
        out_specs=vmem,
        compiler_params=pltpu.CompilerParams(vmem_limit_bytes=12 * 2**20),
        cost_estimate=pl.CostEstimate(
            flops=12 * count * features * units,
            bytes_accessed=12 * features * units,
            transcendentals=2 * count * units,
        ),
        name="expert",
    )(rows, *mine, *theirs)


def logits_kernel(*refs, sizes):
    count = len(sizes)
    pieces, wanted, head = refs[:count], refs[count], refs[count + 1]
    out, stacked, logits = refs[count + 2 :]
    at = 0
    for piece, size in zip(pieces, sizes):
        stacked[at : at + size, :] = piece[...]
        at += size
    half = head.shape[1] // 2
    for cols in (slice(0, half), slice(half, 2 * half)):
        logits[:, cols] = dot(stacked[...], head[:, cols])
    step = 64

    def some_rows(i, carry):
        here = pl.ds(pl.multiple_of(i * step, step), step)
        values = logits[here, :]
        peak = jnp.max(values, axis=1, keepdims=True)
        mass = jnp.sum(jnp.exp(values - peak), axis=1, keepdims=True)
        lane = lax.broadcasted_iota(I32, values.shape, 1)
        hit = jnp.sum(jnp.where(lane == wanted[here, :], values, 0.0), axis=1, keepdims=True)
        slot = lax.broadcasted_iota(I32, (step, 128), 1)
        out[here, :] = jnp.where(slot == 0, peak + jnp.log(mass), hit)
        return carry

    lax.fori_loop(0, at // step, some_rows, 0)


def logits_part(pieces, wanted, head):
    sizes = [piece.shape[0] for piece in pieces]
    count = sum(sizes)
    features, entries = head.shape
    vmem = pl.BlockSpec(memory_space=pltpu.VMEM)
    return pl.pallas_call(
        lambda *refs: logits_kernel(*refs, sizes=sizes),
        out_shape=jax.ShapeDtypeStruct((count, 128), F32),
        in_specs=[vmem] * (len(pieces) + 2),
        out_specs=vmem,
        scratch_shapes=[pltpu.VMEM((count, features), BF), pltpu.VMEM((count, entries), F32)],
        compiler_params=pltpu.CompilerParams(vmem_limit_bytes=10 * 2**20),
        cost_estimate=pl.CostEstimate(
            flops=2 * count * features * entries,
            bytes_accessed=2 * features * entries,
            transcendentals=count * entries,
        ),
        name="logits",
    )(*pieces, wanted.reshape(count, 1), head)


def on_device(
    rollout_states,
    lengths,
    group_ids,
    route_ids,
    route_weights,
    gain_in,
    w_gate,
    w_up,
    w_down,
    gain_out,
    head_weight,
    targets,
    policy_logp,
):
    own_x, own_z, own_y, own_c = (lax.axis_index(a) for a in ("dp", "z", "y", "c"))
    rows, pos_count, features = rollout_states.shape[1:]
    tokens = rows * pos_count
    wide = pos_count * features
    facts = jnp.pad(jnp.stack([group_ids, lengths], axis=1).astype(BF), ((0, 0), (0, 126)))
    block = jnp.concatenate([rollout_states.reshape(rows, wide), facts], axis=1)
    blocks = [block, shift(block, "dp", 1), shift(block, "dp", 2), shift(block, "dp", -1)]
    every = jnp.concatenate(blocks, axis=0)
    every, w_gate, w_up, w_down = lax.optimization_barrier((every, w_gate, w_up, w_down))
    local = jnp.arange(rows, dtype=I32)
    ids = jnp.concatenate([((own_x - k) % NX) * rows + local for k in range(NX)])
    owner = every[:, wide].astype(I32) % NX
    before = (owner[None, :] == owner[:, None]) & (ids[None, :] < ids[:, None])
    rank = jnp.sum(before.astype(I32), axis=1)
    place = jnp.where(owner == own_x, rank, rows)
    pick = (place[None, :] == local[:, None]).astype(BF)
    owned = dot(pick, every)
    owned_lengths = owned[:, wide + 1].astype(I32)
    states_wide = owned[:, :wide].reshape(tokens, features)
    mine = (w_gate[0], w_up[0], w_down[0])
    theirs = []
    for part in mine:
        theirs.append(pair_swap(part, 0))
    normed_in = scaled_norm(states_wide, gain_in).astype(BF)
    target = targets.reshape(tokens, 1)
    info = [route_ids.reshape(tokens, -1).astype(F32)]
    info += three_parts(route_weights.reshape(tokens, -1))
    info += three_parts(policy_logp.reshape(tokens, 1))
    info += [(target // 256).astype(F32), (target % 256).astype(F32)]
    info = jnp.concatenate(info, axis=1)
    width = info.shape[1]
    info = jnp.pad(info, ((0, 0), (0, 128 - width))).astype(BF)
    own = jnp.concatenate([normed_in, info], axis=1)
    up, down = [own], [own]
    for step in range(4):
        up.append(shift(up[-1], "z", 1))
        if step < 3:
            down.append(shift(down[-1], "z", -1))
    ring = up + down[:0:-1]
    topk = route_ids.shape[-1]
    halves = []
    for dzs in HALVES:
        rows_in = jnp.concatenate([ring[dz] for dz in dzs], axis=0)
        count = rows_in.shape[0]
        facts = plain(rows_in[:, features:]).astype(F32)
        named = facts[:, :topk].astype(I32) - own_z * PLANE
        named = named[:, :, None] == jnp.arange(PLANE, dtype=I32)
        member = jnp.any(named, axis=1)
        t = np.arange(count)
        earlier = (t[:, None] // tokens == t[None, :] // tokens) & (t[None, :] < t[:, None])
        rank = dot(jnp.asarray(earlier, BF), member.astype(BF)).astype(I32)
        slot = jnp.where(member, rank + jnp.asarray(t[:, None] // tokens * SLOT, I32), -1)
        spots = len(dzs) * SLOT
        at = jnp.arange(spots, dtype=I32)
        spread = (slot.T[:, None, :] == at[None, :, None]).reshape(PLANE * spots, count)
        sender = dot(spread.astype(BF), rows_in[:, :features]).astype(BF)
        holds = slot[:, :, None] == at
        parts = []
        for k in range(3):
            part = facts[:, topk * (k + 1) : topk * (k + 2)]
            part = jnp.sum(jnp.where(named, part[:, :, None], 0.0), axis=1)
            part = jnp.where(holds, part[:, :, None], 0.0)
            parts.append(part.reshape(count, PLANE * spots).astype(BF))
        arrived = lax.all_to_all(
            sender.reshape(PLANE, spots, features), ("y", "c"), 0, 0, tiled=True
        ).reshape(-1, features)
        paired_rows = pair_swap(arrived, 1)
        halves.append((dzs, spots, parts, arrived, paired_rows))
    facts = jnp.concatenate([plain(block[:, features:]) for block in ring], axis=0).astype(F32)
    policy = facts[:, 4 * topk] + facts[:, 4 * topk + 1] + facts[:, 4 * topk + 2]
    column = jnp.stack([facts[:, width - 2] * 256 + facts[:, width - 1], policy])
    from_pair, own_part = [], []
    for index, half in enumerate(halves):
        for_pair = expert_part(half[4], mine, theirs)
        if index == 0:
            for_pair, column, own = lax.optimization_barrier((for_pair, column, half[3]))
        else:
            for_pair, own = lax.optimization_barrier((for_pair, half[3]))
        from_pair.append(pair_swap(for_pair, 1))
        own_part.append(expert_part(own, mine, theirs))
    plane = sent_to_all(column, ("y", "c")).reshape(NY, NC, 2, NZ, tokens)
    plane_targets, plane_policy = plane[:, :, 0].astype(I32), plane[:, :, 1]
    routed = 0.0
    for index, (dzs, spots, parts, arrived, _) in enumerate(halves):
        own, peer = own_part[index], from_pair[index]
        if index == 0:
            own, plane_targets, plane_policy = lax.optimization_barrier(
                (own, plane_targets, plane_policy)
            )
        else:
            own, peer, worked = lax.optimization_barrier((own, peer, worked))
        worked = (own + peer).astype(BF)
        returned = lax.all_to_all(
            worked.reshape(PLANE, spots, features), ("y", "c"), 0, 0, tiled=True
        ).reshape(-1, features)
        partial = sum(dot(part, returned) for part in parts)
        for i, dz in enumerate(dzs):
            share = partial[i * tokens : (i + 1) * tokens]
            if dz:
                share = shift(share, "z", -dz)
            routed = routed + share
    mixed_sum = states_wide + routed
    final_rows = scaled_norm(mixed_sum, gain_out).astype(BF)
    right = shift(final_rows, "y", 1)
    left = shift(final_rows, "y", -1)
    far = shift(right, "y", 1)
    col = jnp.concatenate([final_rows, right, far, left], axis=0)
    chunks = [([0], [col])]
    u, d = col, col
    for k in range(1, 4):
        u, d = shift(u, "z", 1), shift(d, "z", -1)
        chunks.append(([k, NZ - k], [u, d]))
    half = u.shape[0] // 2
    chunks.append(([4], [shift(u[:half], "z", 1), shift(d[half:], "z", -1)]))
    chunks[:2] = [(chunks[0][0] + chunks[1][0], chunks[0][1] + chunks[1][1])]
    vocab_part = head_weight.shape[1]
    own_expert = (own_z * NY + own_y) * NC + own_c
    vocab_start = own_expert * vocab_part
    by_dy = turned(plane_targets, own_y, NY)
    by_place = turned(by_dy.transpose(1, 2, 0, 3), own_c, NC)
    found = {}
    for dzs, pieces in chunks:
        other = [shift(piece, "c", 1) for piece in pieces]
        wanted = jnp.stack([by_place[dc, dz] for dc in range(NC) for dz in dzs]).reshape(-1)
        two = logits_part(pieces + other, wanted - vocab_start, head_weight)[:, :2]
        two = two.T.reshape(2, NC, len(dzs), NY, tokens)
        for i, dz in enumerate(dzs):
            found[dz] = two[:, :, i]
    stats = jnp.stack([found[dz] for dz in range(NZ)], axis=2)
    stats = turned(stats.transpose(2, 3, 1, 0, 4), own_z, NZ)
    stats = turned(stats.transpose(1, 0, 2, 3, 4), own_y, NY)
    stats = turned(stats.transpose(2, 1, 0, 3, 4), own_c, NC)
    stats = stats.transpose(3, 1, 2, 0, 4).reshape(2, -1)
    many = sent_to_all(stats, EXPERT)
    peak = jnp.max(many[:, 0], axis=0)
    mass = jnp.sum(jnp.exp(many[:, 0] - peak[None]), axis=0)
    ref_logp = jnp.sum(many[:, 1], axis=0) - (peak + jnp.log(mass))
    policy = turned(plane_policy.transpose(2, 0, 1, 3), own_z, NZ).reshape(-1)
    log_ratio = jnp.clip(ref_logp - policy, -10.0, 10.0)
    token_value = (jnp.exp(log_ratio) - log_ratio - 1.0).reshape(-1, rows, pos_count)
    at = jnp.arange(NZ * PLANE, dtype=I32)
    position = at[:, None] * pos_count + jnp.arange(pos_count, dtype=I32)[None, :]
    inside = position[:, None, :] < owned_lengths[None, :, None]
    all_kl = jnp.where(inside, token_value, 0.0)
    token_kl = jnp.sum(jnp.where((at == own_expert)[:, None, None], all_kl, 0.0), axis=0)
    row_kl = jnp.sum(all_kl, axis=(0, 2)) / owned_lengths.astype(F32)
    return (token_kl.reshape(1, rows, pos_count), row_kl)


def solution(mesh):
    cut = Mesh(mesh.devices.reshape(NX, NZ, NY, NC), ("dp", *EXPERT))
    in_specs = (
        P(EXPERT, "dp", None, None),
        P("dp"),
        P("dp"),
        P(EXPERT, "dp", None, None),
        P(EXPERT, "dp", None, None),
        P(),
        P(EXPERT, None, "dp"),
        P(EXPERT, None, "dp"),
        P(EXPERT, "dp", None),
        P(),
        P(None, EXPERT),
        P(EXPERT, "dp", None),
        P(EXPERT, "dp", None),
    )
    out_specs = (P(EXPERT, "dp", None), P("dp"))
    return jax.shard_map(on_device, mesh=cut, in_specs=in_specs, out_specs=out_specs, check_vma=False)
```

```python
import jax
import jax.numpy as jnp
import numpy as np
from jax import lax
from jax.experimental import pallas as pl
from jax.experimental.pallas import tpu as pltpu
from jax.sharding import Mesh
from jax.sharding import PartitionSpec as P

BF = jnp.bfloat16
F32 = jnp.float32
I32 = jnp.int32
NX, NZ, NY, NC = 4, 8, 4, 2
PLANE = NY * NC
EXPERTS = NZ * PLANE
HALF = 2
EXPERT = ("z", "y", "c")


def shift(value, axis, by):
    size = {"dp": NX, "z": NZ, "y": NY, "c": NC}[axis]
    return lax.ppermute(value, axis, [(i, (i + by) % size) for i in range(size)])


def pair_swap(value, parity):
    perm = []
    for x in range(NX):
        for e in range(NZ * NY * NC):
            if (e % NC + parity) % 2 == 0:
                peer = x ^ 1
            else:
                peer = (x + 1) % NX if x % 2 else (x - 1) % NX
            perm.append((x * NZ * PLANE + e, peer * NZ * PLANE + e))
    return lax.ppermute(value, ("dp", *EXPERT), perm)


def sent_to_all(value, axis):
    copies = jnp.broadcast_to(value, (lax.axis_size(axis), *value.shape))
    return lax.all_to_all(copies, axis, split_axis=0, concat_axis=0, tiled=True)


def turned(value, own, size):
    at = jnp.arange(size, dtype=I32)
    one = (own - at[:, None]) % size == at[None, :]
    one = one.reshape(size, size, *([1] * (value.ndim - 1)))
    return jnp.sum(jnp.where(one, value[None], jnp.zeros((), value.dtype)), axis=1)


def scaled_norm(values, gain_vec):
    mean_square = jnp.mean(values * values, axis=-1, keepdims=True)
    return values * lax.rsqrt(mean_square + 1e-06) * gain_vec


def dot(a, b):
    return jnp.dot(a, b, preferred_element_type=F32)


def three_parts(value):
    parts = []
    for _ in range(3):
        part = lax.reduce_precision(value, 8, 7)
        parts.append(part)
        value = value - part
    return parts


def expert_kernel(*refs):
    rows, weights = refs[0], refs[1:7]
    out, gate, up, down, sems = refs[7:]
    buffers = (gate, up, down)
    order = [(0, 0), (1, 0), (0, 1), (1, 1), (2, 0), (2, 1)]
    copies = {}
    for kind, side in order:
        copies[kind, side] = pltpu.make_async_copy(
            weights[side * 3 + kind], buffers[kind].at[side], sems.at[side * 3 + kind]
        )
        copies[kind, side].start()
    hidden = []
    for side in range(2):
        copies[0, side].wait()
        gated = dot(rows[...], gate[side])
        copies[1, side].wait()
        hidden.append((gated * jax.nn.sigmoid(gated) * dot(rows[...], up[side])).astype(BF))
    copies[2, 0].wait()
    copies[2, 1].wait()
    step = 1024
    for at in range(0, out.shape[1], step):
        cols = slice(at, at + step)
        out[:, cols] = dot(hidden[0], down[0, :, cols]) + dot(hidden[1], down[1, :, cols])


def expert_part(rows, mine, theirs):
    features, units = mine[0].shape
    count = rows.shape[0]
    vmem = pl.BlockSpec(memory_space=pltpu.VMEM)
    flops = 12 * count * features * units
    return pl.pallas_call(
        expert_kernel,
        out_shape=jax.ShapeDtypeStruct(rows.shape, F32),
        in_specs=[vmem] + [pl.BlockSpec(memory_space=pl.ANY)] * 6,
        out_specs=vmem,
        scratch_shapes=[
            pltpu.VMEM((2, features, units), BF),
            pltpu.VMEM((2, features, units), BF),
            pltpu.VMEM((2, units, features), BF),
            pltpu.SemaphoreType.DMA((6,)),
        ],
        compiler_params=pltpu.CompilerParams(vmem_limit_bytes=40 * 2**20),
        cost_estimate=pl.CostEstimate(
            flops=flops, bytes_accessed=12 * features * units, transcendentals=2 * count * units
        ),
        name="expert",
    )(rows, *mine, *theirs)


def logits_kernel(*refs, sizes):
    count = len(sizes)
    pieces, wanted, head = refs[:count], refs[count], refs[count + 1]
    out, stacked, logits = refs[count + 2 :]
    at = 0
    for piece, size in zip(pieces, sizes):
        stacked[at : at + size, :] = piece[...]
        at += size
    half = head.shape[1] // 2
    for cols in (slice(0, half), slice(half, 2 * half)):
        logits[:, cols] = dot(stacked[...], head[:, cols])
    step = 64

    def some_rows(i, carry):
        here = pl.ds(pl.multiple_of(i * step, step), step)
        values = logits[here, :]
        peak = jnp.max(values, axis=1, keepdims=True)
        mass = jnp.sum(jnp.exp(values - peak), axis=1, keepdims=True)
        lane = lax.broadcasted_iota(I32, values.shape, 1)
        hit = jnp.sum(jnp.where(lane == wanted[here, :], values, 0.0), axis=1, keepdims=True)
        slot = lax.broadcasted_iota(I32, (step, 128), 1)
        out[here, :] = jnp.where(slot == 0, peak + jnp.log(mass), hit)
        return carry

    lax.fori_loop(0, at // step, some_rows, 0)


def logits_part(pieces, wanted, head):
    sizes = [piece.shape[0] for piece in pieces]
    count = sum(sizes)
    features, entries = head.shape
    vmem = pl.BlockSpec(memory_space=pltpu.VMEM)
    return pl.pallas_call(
        lambda *refs: logits_kernel(*refs, sizes=sizes),
        out_shape=jax.ShapeDtypeStruct((count, 128), F32),
        in_specs=[vmem] * (len(pieces) + 2),
        out_specs=vmem,
        scratch_shapes=[pltpu.VMEM((count, features), BF), pltpu.VMEM((count, entries), F32)],
        compiler_params=pltpu.CompilerParams(vmem_limit_bytes=10 * 2**20),
        cost_estimate=pl.CostEstimate(
            flops=2 * count * features * entries,
            bytes_accessed=2 * features * entries,
            transcendentals=count * entries,
        ),
        name="logits",
    )(*pieces, wanted.reshape(count, 1), head)


def on_device(
    rollout_states,
    lengths,
    group_ids,
    route_ids,
    route_weights,
    gain_in,
    w_gate,
    w_up,
    w_down,
    gain_out,
    head_weight,
    targets,
    policy_logp,
):
    own_x, own_z, own_y, own_c = (lax.axis_index(a) for a in ("dp", "z", "y", "c"))
    rows, pos_count, features = rollout_states.shape[1:]
    tokens = rows * pos_count
    wide = pos_count * features
    facts = jnp.pad(jnp.stack([group_ids, lengths], axis=1).astype(BF), ((0, 0), (0, 126)))
    block = jnp.concatenate([rollout_states.reshape(rows, wide), facts], axis=1)
    blocks = [block, shift(block, "dp", 1), shift(block, "dp", 2), shift(block, "dp", -1)]
    every = jnp.concatenate(blocks, axis=0)
    every, w_gate, w_up, w_down = lax.optimization_barrier((every, w_gate, w_up, w_down))
    local = jnp.arange(rows, dtype=I32)
    ids = jnp.concatenate([((own_x - k) % NX) * rows + local for k in range(NX)])
    owner = every[:, wide].astype(I32) % NX
    before = (owner[None, :] == owner[:, None]) & (ids[None, :] < ids[:, None])
    rank = jnp.sum(before.astype(I32), axis=1)
    place = jnp.where(owner == own_x, rank, rows)
    pick = (place[None, :] == local[:, None]).astype(BF)
    owned = dot(pick, every)
    owned_lengths = owned[:, wide + 1].astype(I32)
    states_wide = owned[:, :wide].reshape(tokens, features)
    mine = (w_gate[0], w_up[0], w_down[0])
    theirs = []
    for part in mine:
        theirs.append(pair_swap(part, 0))
    normed_in = scaled_norm(states_wide, gain_in).astype(BF)
    expert_ids = route_ids.reshape(tokens, -1)
    gates = route_weights.reshape(tokens, -1)
    named = expert_ids[:, :, None] == jnp.arange(EXPERTS, dtype=I32)
    member = jnp.any(named, axis=1)
    weight = jnp.sum(jnp.where(named, gates[:, :, None], 0.0), axis=1)
    t = np.arange(tokens)
    earlier = jnp.asarray(t[None, :] < t[:, None], BF)
    rank = jnp.where(member, dot(earlier, member.astype(BF)).astype(I32), -1)
    halves = []
    for index in range(2):
        at = jnp.arange(HALF, dtype=I32) + index * HALF
        spread = (rank.T[:, None, :] == at[None, :, None]).reshape(EXPERTS * HALF, tokens)
        sender = dot(spread.astype(BF), normed_in).astype(BF)
        arrived = lax.all_to_all(
            sender.reshape(EXPERTS, HALF, features), EXPERT, 0, 0, tiled=True
        ).reshape(-1, features)
        paired_rows = pair_swap(arrived, 1)
        holds = rank[:, :, None] == at
        held = jnp.where(holds, weight[:, :, None], 0.0).reshape(tokens, EXPERTS * HALF)
        parts = jnp.concatenate(three_parts(held), axis=0).astype(BF)
        halves.append((parts, arrived, paired_rows))
    facts = jnp.stack([targets.reshape(tokens).astype(F32), policy_logp.reshape(tokens)])
    from_pair, own_part = [], []
    for index, (_, own, paired_rows) in enumerate(halves):
        for_pair = expert_part(paired_rows, mine, theirs)
        for_pair, own, facts = lax.optimization_barrier((for_pair, own, facts))
        from_pair.append(pair_swap(for_pair, 1))
        own_part.append(expert_part(own, mine, theirs))
        if index == 0:
            every_fact = sent_to_all(facts, EXPERT).reshape(NZ, NY, NC, 2, tokens)
    all_targets, all_policy = every_fact[:, :, :, 0].astype(I32), every_fact[:, :, :, 1]
    routed = 0.0
    for index, (parts, _, _) in enumerate(halves):
        own, peer = own_part[index], from_pair[index]
        if index == 0:
            own, all_targets, all_policy = lax.optimization_barrier((own, all_targets, all_policy))
        else:
            own, peer, worked = lax.optimization_barrier((own, peer, worked))
        worked = (own + peer).astype(BF)
        if index:
            worked, returned = lax.optimization_barrier((worked, returned))
        returned = lax.all_to_all(
            worked.reshape(EXPERTS, HALF, features), EXPERT, 0, 0, tiled=True
        ).reshape(-1, features)
        share = dot(parts, returned).reshape(3, tokens, features)
        routed = routed + share[0] + share[1] + share[2]
    mixed_sum = states_wide + routed
    final_rows = scaled_norm(mixed_sum, gain_out).astype(BF)
    right = shift(final_rows, "y", 1)
    left = shift(final_rows, "y", -1)
    far = shift(right, "y", 1)
    col = jnp.concatenate([final_rows, right, far, left], axis=0)
    chunks = [([0], [col])]
    u, d = col, col
    for k in range(1, 4):
        u, d = shift(u, "z", 1), shift(d, "z", -1)
        chunks.append(([k, NZ - k], [u, d]))
    half = u.shape[0] // 2
    chunks.append(([4], [shift(u[:half], "z", 1), shift(d[half:], "z", -1)]))
    for k in (3, 0):
        chunks[k : k + 2] = [tuple(a + b for a, b in zip(chunks[k], chunks[k + 1]))]
    vocab_part = head_weight.shape[1]
    own_expert = (own_z * NY + own_y) * NC + own_c
    vocab_start = own_expert * vocab_part
    by_place = turned(all_targets, own_z, NZ)
    by_place = turned(by_place.transpose(1, 0, 2, 3), own_y, NY)
    by_place = turned(by_place.transpose(2, 1, 0, 3), own_c, NC)
    found = {}
    for dzs, pieces in chunks:
        other = [shift(piece, "c", 1) for piece in pieces]
        wanted = jnp.stack([by_place[dc, dz] for dc in range(NC) for dz in dzs]).reshape(-1)
        two = logits_part(pieces + other, wanted - vocab_start, head_weight)[:, :2]
        two = two.T.reshape(2, NC, len(dzs), NY, tokens)
        for i, dz in enumerate(dzs):
            found[dz] = two[:, :, i]
    stats = jnp.stack([found[dz] for dz in range(NZ)], axis=2)
    stats = turned(stats.transpose(2, 3, 1, 0, 4), own_z, NZ)
    stats = turned(stats.transpose(1, 0, 2, 3, 4), own_y, NY)
    stats = turned(stats.transpose(2, 1, 0, 3, 4), own_c, NC)
    stats = stats.transpose(3, 1, 2, 0, 4).reshape(2, -1)
    many = sent_to_all(stats, EXPERT)
    peak = jnp.max(many[:, 0], axis=0)
    mass = jnp.sum(jnp.exp(many[:, 0] - peak[None]), axis=0)
    ref_logp = jnp.sum(many[:, 1], axis=0) - (peak + jnp.log(mass))
    log_ratio = jnp.clip(ref_logp - all_policy.reshape(-1), -10.0, 10.0)
    token_value = (jnp.exp(log_ratio) - log_ratio - 1.0).reshape(-1, rows, pos_count)
    at = jnp.arange(NZ * PLANE, dtype=I32)
    position = at[:, None] * pos_count + jnp.arange(pos_count, dtype=I32)[None, :]
    inside = position[:, None, :] < owned_lengths[None, :, None]
    all_kl = jnp.where(inside, token_value, 0.0)
    token_kl = jnp.sum(jnp.where((at == own_expert)[:, None, None], all_kl, 0.0), axis=0)
    row_kl = jnp.sum(all_kl, axis=(0, 2)) / owned_lengths.astype(F32)
    return (token_kl.reshape(1, rows, pos_count), row_kl)


def solution(mesh):
    cut = Mesh(mesh.devices.reshape(NX, NZ, NY, NC), ("dp", *EXPERT))
    in_specs = (
        P(EXPERT, "dp", None, None),
        P("dp"),
        P("dp"),
        P(EXPERT, "dp", None, None),
        P(EXPERT, "dp", None, None),
        P(),
        P(EXPERT, None, "dp"),
        P(EXPERT, None, "dp"),
        P(EXPERT, "dp", None),
        P(),
        P(None, EXPERT),
        P(EXPERT, "dp", None),
        P(EXPERT, "dp", None),
    )
    out_specs = (P(EXPERT, "dp", None), P("dp"))
    return jax.shard_map(on_device, mesh=cut, in_specs=in_specs, out_specs=out_specs, check_vma=False)
```

```python
import jax
import jax.numpy as jnp
import numpy as np
from jax import lax
from jax.experimental import pallas as pl
from jax.experimental.layout import Layout, with_layout_constraint
from jax.experimental.pallas import tpu as pltpu
from jax.sharding import Mesh
from jax.sharding import PartitionSpec as P

BF = jnp.bfloat16
F32 = jnp.float32
I32 = jnp.int32
NX, NZ, NY, NC = 4, 8, 4, 2
PLANE = NY * NC
SLOT = 4
EXPERT = ("z", "y", "c")


def shift(value, axis, by):
    size = {"dp": NX, "z": NZ, "y": NY, "c": NC}[axis]
    return lax.ppermute(value, axis, [(i, (i + by) % size) for i in range(size)])


def pair_swap(value, parity):
    perm = []
    for x in range(NX):
        for e in range(NZ * NY * NC):
            if (e % NC + parity) % 2 == 0:
                peer = x ^ 1
            else:
                peer = (x + 1) % NX if x % 2 else (x - 1) % NX
            perm.append((x * NZ * PLANE + e, peer * NZ * PLANE + e))
    return lax.ppermute(value, ("dp", *EXPERT), perm)


def sent_to_all(value, axis):
    copies = jnp.broadcast_to(value, (lax.axis_size(axis), *value.shape))
    return lax.all_to_all(copies, axis, split_axis=0, concat_axis=0, tiled=True)


def turned(value, own, size):
    at = jnp.arange(size, dtype=I32)
    one = (own - at[:, None]) % size == at[None, :]
    one = one.reshape(size, size, *([1] * (value.ndim - 1)))
    return jnp.sum(jnp.where(one, value[None], jnp.zeros((), value.dtype)), axis=1)


def scaled_norm(values, gain_vec):
    mean_square = jnp.mean(values * values, axis=-1, keepdims=True)
    return values * lax.rsqrt(mean_square + 1e-06) * gain_vec


def plain(value):
    return with_layout_constraint(value, Layout(tuple(range(value.ndim))))


def dot(a, b):
    return jnp.dot(a, b, preferred_element_type=F32)


def three_parts(value):
    parts = []
    for _ in range(3):
        part = lax.reduce_precision(value, 8, 7)
        parts.append(part)
        value = value - part
    return parts


def expert_kernel(rows, gate_0, up_0, down_0, gate_1, up_1, down_1, out):
    count, features = rows.shape
    units = gate_0.shape[1]
    step = features // 8

    def some_features(i, sums):
        here = pl.ds(pl.multiple_of(i * step, step), step)
        given = rows[:, here]
        parts = [dot(given, ref[here, :]) for ref in (gate_0, up_0, gate_1, up_1)]
        return tuple(s + p for s, p in zip(sums, parts))

    zero = jnp.zeros((count, units), F32)
    gated_0, upped_0, gated_1, upped_1 = lax.fori_loop(0, 8, some_features, (zero,) * 4)
    hidden_0 = (gated_0 * jax.nn.sigmoid(gated_0) * upped_0).astype(BF)
    hidden_1 = (gated_1 * jax.nn.sigmoid(gated_1) * upped_1).astype(BF)

    def some_outputs(i, carry):
        cols = pl.ds(pl.multiple_of(i * step, step), step)
        out[:, cols] = dot(hidden_0, down_0[:, cols]) + dot(hidden_1, down_1[:, cols])
        return carry

    lax.fori_loop(0, 8, some_outputs, 0)


def expert_part(rows, mine, theirs):
    features, units = mine[0].shape
    count = rows.shape[0]
    vmem = pl.BlockSpec(memory_space=pltpu.VMEM)
    return pl.pallas_call(
        expert_kernel,
        out_shape=jax.ShapeDtypeStruct(rows.shape, F32),
        in_specs=[vmem] * 7,
        out_specs=vmem,
        compiler_params=pltpu.CompilerParams(vmem_limit_bytes=12 * 2**20),
        cost_estimate=pl.CostEstimate(
            flops=12 * count * features * units,
            bytes_accessed=12 * features * units,
            transcendentals=2 * count * units,
        ),
        name="expert",
    )(rows, *mine, *theirs)


def logits_kernel(*refs, sizes):
    count = len(sizes)
    pieces, wanted, head = refs[:count], refs[count], refs[count + 1]
    out, stacked, logits = refs[count + 2 :]
    at = 0
    for piece, size in zip(pieces, sizes):
        stacked[at : at + size, :] = piece[...]
        at += size
    part = head.shape[1] // 4

    def some_entries(i, carry):
        cols = pl.ds(pl.multiple_of(i * part, part), part)
        logits[:, cols] = dot(stacked[...], head[:, cols])
        return carry

    lax.fori_loop(0, 4, some_entries, 0)
    step = 64

    def some_rows(i, carry):
        here = pl.ds(pl.multiple_of(i * step, step), step)
        values = logits[here, :]
        peak = jnp.max(values, axis=1, keepdims=True)
        mass = jnp.sum(jnp.exp(values - peak), axis=1, keepdims=True)
        lane = lax.broadcasted_iota(I32, values.shape, 1)
        hit = jnp.sum(jnp.where(lane == wanted[here, :], values, 0.0), axis=1, keepdims=True)
        slot = lax.broadcasted_iota(I32, (step, 128), 1)
        out[here, :] = jnp.where(slot == 0, peak + jnp.log(mass), hit)
        return carry

    lax.fori_loop(0, at // step, some_rows, 0)


def logits_part(pieces, wanted, head):
    sizes = [piece.shape[0] for piece in pieces]
    count = sum(sizes)
    features, entries = head.shape
    vmem = pl.BlockSpec(memory_space=pltpu.VMEM)
    return pl.pallas_call(
        lambda *refs: logits_kernel(*refs, sizes=sizes),
        out_shape=jax.ShapeDtypeStruct((count, 128), F32),
        in_specs=[vmem] * (len(pieces) + 2),
        out_specs=vmem,
        scratch_shapes=[pltpu.VMEM((count, features), BF), pltpu.VMEM((count, entries), F32)],
        compiler_params=pltpu.CompilerParams(vmem_limit_bytes=10 * 2**20),
        cost_estimate=pl.CostEstimate(
            flops=2 * count * features * entries,
            bytes_accessed=2 * features * entries,
            transcendentals=count * entries,
        ),
        name="logits",
    )(*pieces, wanted.reshape(count, 1), head)


def on_device(
    rollout_states,
    lengths,
    group_ids,
    route_ids,
    route_weights,
    gain_in,
    w_gate,
    w_up,
    w_down,
    gain_out,
    head_weight,
    targets,
    policy_logp,
):
    own_x, own_z, own_y, own_c = (lax.axis_index(a) for a in ("dp", "z", "y", "c"))
    rows, pos_count, features = rollout_states.shape[1:]
    tokens = rows * pos_count
    wide = pos_count * features
    facts = jnp.pad(jnp.stack([group_ids, lengths], axis=1).astype(BF), ((0, 0), (0, 126)))
    block = jnp.concatenate([rollout_states.reshape(rows, wide), facts], axis=1)
    blocks = [block, shift(block, "dp", 1), shift(block, "dp", 2), shift(block, "dp", -1)]
    every = jnp.concatenate(blocks, axis=0)
    every, w_gate, w_up, w_down = lax.optimization_barrier((every, w_gate, w_up, w_down))
    local = jnp.arange(rows, dtype=I32)
    ids = jnp.concatenate([((own_x - k) % NX) * rows + local for k in range(NX)])
    owner = every[:, wide].astype(I32) % NX
    before = (owner[None, :] == owner[:, None]) & (ids[None, :] < ids[:, None])
    rank = jnp.sum(before.astype(I32), axis=1)
    place = jnp.where(owner == own_x, rank, rows)
    pick = (place[None, :] == local[:, None]).astype(BF)
    owned = dot(pick, every)
    owned_lengths = owned[:, wide + 1].astype(I32)
    states_wide = owned[:, :wide].reshape(tokens, features)
    mine = (w_gate[0], w_up[0], w_down[0])
    theirs = []
    for part in mine:
        theirs.append(pair_swap(part, 0))
    normed_in = scaled_norm(states_wide, gain_in).astype(BF)
    target = targets.reshape(tokens, 1)
    expert_ids = route_ids.reshape(tokens, -1)
    topk = expert_ids.shape[1]
    info = [expert_ids.astype(F32)]
    info += three_parts(policy_logp.reshape(tokens, 1))
    info += [(target // 256).astype(F32), (target % 256).astype(F32)]
    info = jnp.concatenate(info, axis=1)
    info = jnp.pad(info, ((0, 0), (0, 128 - info.shape[1]))).astype(BF)
    own = jnp.concatenate([normed_in, info], axis=1)
    every_z = sent_to_all(own, "z")
    halves = []
    for index in range(2):
        blocks = NZ // 2
        rows_in = every_z[index * blocks : (index + 1) * blocks].reshape(blocks * tokens, -1)
        count = rows_in.shape[0]
        ids = plain(rows_in[:, features:]).astype(F32)[:, :topk].astype(I32) - own_z * PLANE
        member = jnp.any(ids[:, :, None] == jnp.arange(PLANE, dtype=I32), axis=1)
        t = np.arange(count)
        earlier = (t[:, None] // tokens == t[None, :] // tokens) & (t[None, :] < t[:, None])
        rank = dot(jnp.asarray(earlier, BF), member.astype(BF)).astype(I32)
        slot = jnp.where(member, rank + jnp.asarray(t[:, None] // tokens * SLOT, I32), -1)
        spots = blocks * SLOT
        at = jnp.arange(spots, dtype=I32)
        spread = (slot.T[:, None, :] == at[None, :, None]).reshape(PLANE * spots, count)
        sender = dot(spread.astype(BF), rows_in[:, :features]).astype(BF)
        arrived = lax.all_to_all(
            sender.reshape(PLANE, spots, features), ("y", "c"), 0, 0, tiled=True
        ).reshape(-1, features)
        paired_rows = pair_swap(arrived, 1)
        halves.append((arrived, paired_rows))
    facts = plain(every_z[:, :, features:]).astype(F32)
    policy = facts[:, :, topk] + facts[:, :, topk + 1] + facts[:, :, topk + 2]
    column = jnp.stack([facts[:, :, topk + 3] * 256 + facts[:, :, topk + 4], policy])
    column = column.reshape(2, NZ * tokens)
    from_pair, own_part = [], []
    for index, (own, paired_rows) in enumerate(halves):
        for_pair = expert_part(paired_rows, mine, theirs)
        for_pair, own, column = lax.optimization_barrier((for_pair, own, column))
        from_pair.append(pair_swap(for_pair, 1))
        own_part.append(expert_part(own, mine, theirs))
        if index == 0:
            plane = sent_to_all(column, ("y", "c")).reshape(NY, NC, 2, NZ, tokens)
    all_targets = plane[:, :, 0].astype(I32).transpose(2, 0, 1, 3)
    all_policy = plane[:, :, 1].transpose(2, 0, 1, 3)
    blocks = NZ // 2
    order = np.arange(NZ * PLANE * SLOT).reshape(2, PLANE, blocks, SLOT)
    order = order.transpose(0, 2, 1, 3).reshape(-1)
    sort = order[:, None] == np.arange(len(order))[None, :]
    worked = []
    for own, peer in zip(own_part, from_pair):
        if worked:
            own, peer, *_ = lax.optimization_barrier((own, peer, worked[0]))
        else:
            own, all_targets, all_policy = lax.optimization_barrier((own, all_targets, all_policy))
        worked.append((own + peer).astype(BF))
    cut = len(order) // 2
    sort = jnp.asarray(sort, BF)
    home = (dot(sort[:, :cut], worked[0]) + dot(sort[:, cut:], worked[1])).astype(BF)
    returned = lax.all_to_all(
        home.reshape(-1, SLOT, features), EXPERT, 0, 0, tiled=True
    ).reshape(-1, features)
    gates = route_weights.reshape(tokens, -1)
    named = expert_ids[:, :, None] == jnp.arange(NZ * PLANE, dtype=I32)
    member = jnp.any(named, axis=1)
    weight = jnp.sum(jnp.where(named, gates[:, :, None], 0.0), axis=1)
    t = np.arange(tokens)
    rank = dot(jnp.asarray(t[None, :] < t[:, None], BF), member.astype(BF)).astype(I32)
    holds = member[:, :, None] & (rank[:, :, None] == jnp.arange(SLOT, dtype=I32))
    held = jnp.where(holds, weight[:, :, None], 0.0).reshape(tokens, -1)
    share = dot(jnp.concatenate(three_parts(held), axis=0).astype(BF), returned)
    share = share.reshape(3, tokens, features)
    routed = share[0] + share[1] + share[2]
    mixed_sum = states_wide + routed
    final_rows = scaled_norm(mixed_sum, gain_out).astype(BF)
    right = shift(final_rows, "y", 1)
    left = shift(final_rows, "y", -1)
    far = shift(right, "y", 1)
    col = jnp.concatenate([final_rows, right, far, left], axis=0)
    chunks = [([0], [col])]
    u, d = col, col
    for k in range(1, 4):
        u, d = shift(u, "z", 1), shift(d, "z", -1)
        chunks.append(([k, NZ - k], [u, d]))
    half = u.shape[0] // 2
    chunks.append(([4], [shift(u[:half], "z", 1), shift(d[half:], "z", -1)]))
    chunks[:2] = [(chunks[0][0] + chunks[1][0], chunks[0][1] + chunks[1][1])]
    vocab_part = head_weight.shape[1]
    own_expert = (own_z * NY + own_y) * NC + own_c
    vocab_start = own_expert * vocab_part
    by_place = turned(all_targets, own_z, NZ)
    by_place = turned(by_place.transpose(1, 0, 2, 3), own_y, NY)
    by_place = turned(by_place.transpose(2, 1, 0, 3), own_c, NC)
    found = {}
    for dzs, pieces in chunks:
        other = [shift(piece, "c", 1) for piece in pieces]
        wanted = jnp.stack([by_place[dc, dz] for dc in range(NC) for dz in dzs]).reshape(-1)
        two = logits_part(pieces + other, wanted - vocab_start, head_weight)[:, :2]
        two = two.T.reshape(2, NC, len(dzs), NY, tokens)
        for i, dz in enumerate(dzs):
            found[dz] = two[:, :, i]
    stats = jnp.stack([found[dz] for dz in range(NZ)], axis=2)
    stats = turned(stats.transpose(2, 3, 1, 0, 4), own_z, NZ)
    stats = turned(stats.transpose(1, 0, 2, 3, 4), own_y, NY)
    stats = turned(stats.transpose(2, 1, 0, 3, 4), own_c, NC)
    stats = stats.transpose(3, 1, 2, 0, 4).reshape(2, -1)
    many = sent_to_all(stats, EXPERT)
    peak = jnp.max(many[:, 0], axis=0)
    mass = jnp.sum(jnp.exp(many[:, 0] - peak[None]), axis=0)
    ref_logp = jnp.sum(many[:, 1], axis=0) - (peak + jnp.log(mass))
    log_ratio = jnp.clip(ref_logp - all_policy.reshape(-1), -10.0, 10.0)
    token_value = (jnp.exp(log_ratio) - log_ratio - 1.0).reshape(-1, rows, pos_count)
    at = jnp.arange(NZ * PLANE, dtype=I32)
    position = at[:, None] * pos_count + jnp.arange(pos_count, dtype=I32)[None, :]
    inside = position[:, None, :] < owned_lengths[None, :, None]
    all_kl = jnp.where(inside, token_value, 0.0)
    token_kl = jnp.sum(jnp.where((at == own_expert)[:, None, None], all_kl, 0.0), axis=0)
    row_kl = jnp.sum(all_kl, axis=(0, 2)) / owned_lengths.astype(F32)
    return (token_kl.reshape(1, rows, pos_count), row_kl)


def solution(mesh):
    cut = Mesh(mesh.devices.reshape(NX, NZ, NY, NC), ("dp", *EXPERT))
    in_specs = (
        P(EXPERT, "dp", None, None),
        P("dp"),
        P("dp"),
        P(EXPERT, "dp", None, None),
        P(EXPERT, "dp", None, None),
        P(),
        P(EXPERT, None, "dp"),
        P(EXPERT, None, "dp"),
        P(EXPERT, "dp", None),
        P(),
        P(None, EXPERT),
        P(EXPERT, "dp", None),
        P(EXPERT, "dp", None),
    )
    out_specs = (P(EXPERT, "dp", None), P("dp"))
    return jax.shard_map(on_device, mesh=cut, in_specs=in_specs, out_specs=out_specs, check_vma=False)
```

```python
import jax
import jax.numpy as jnp
import numpy as np
from jax import lax
from jax.experimental import pallas as pl
from jax.experimental.layout import Layout, with_layout_constraint
from jax.experimental.pallas import tpu as pltpu
from jax.sharding import Mesh
from jax.sharding import PartitionSpec as P

BF = jnp.bfloat16
F32 = jnp.float32
I32 = jnp.int32
NX, NZ, NY, NC = 4, 8, 4, 2
PLANE = NY * NC
SLOT = 4
EXPERT = ("z", "y", "c")


def shift(value, axis, by):
    size = {"dp": NX, "z": NZ, "y": NY, "c": NC}[axis]
    return lax.ppermute(value, axis, [(i, (i + by) % size) for i in range(size)])


def pair_swap(value, parity):
    perm = []
    for x in range(NX):
        for e in range(NZ * NY * NC):
            if (e % NC + parity) % 2 == 0:
                peer = x ^ 1
            else:
                peer = (x + 1) % NX if x % 2 else (x - 1) % NX
            perm.append((x * NZ * PLANE + e, peer * NZ * PLANE + e))
    return lax.ppermute(value, ("dp", *EXPERT), perm)


def sent_to_all(value, axis):
    copies = jnp.broadcast_to(value, (lax.axis_size(axis), *value.shape))
    return lax.all_to_all(copies, axis, split_axis=0, concat_axis=0, tiled=True)


def turned(value, own, size):
    at = jnp.arange(size, dtype=I32)
    one = (own - at[:, None]) % size == at[None, :]
    one = one.reshape(size, size, *([1] * (value.ndim - 1)))
    return jnp.sum(jnp.where(one, value[None], jnp.zeros((), value.dtype)), axis=1)


def scaled_norm(values, gain_vec):
    mean_square = jnp.mean(values * values, axis=-1, keepdims=True)
    return values * lax.rsqrt(mean_square + 1e-06) * gain_vec


def plain(value):
    return with_layout_constraint(value, Layout(tuple(range(value.ndim))))


def dot(a, b):
    return jnp.dot(a, b, preferred_element_type=F32)


def three_parts(value):
    parts = []
    for _ in range(3):
        part = lax.reduce_precision(value, 8, 7)
        parts.append(part)
        value = value - part
    return parts


def expert_kernel(rows, gate_0, up_0, down_0, gate_1, up_1, down_1, out):
    count, features = rows.shape
    units = gate_0.shape[1]
    step = features // 8

    def some_features(i, sums):
        here = pl.ds(pl.multiple_of(i * step, step), step)
        given = rows[:, here]
        parts = [dot(given, ref[here, :]) for ref in (gate_0, up_0, gate_1, up_1)]
        return tuple(s + p for s, p in zip(sums, parts))

    zero = jnp.zeros((count, units), F32)
    gated_0, upped_0, gated_1, upped_1 = lax.fori_loop(0, 8, some_features, (zero,) * 4)
    hidden_0 = (gated_0 * jax.nn.sigmoid(gated_0) * upped_0).astype(BF)
    hidden_1 = (gated_1 * jax.nn.sigmoid(gated_1) * upped_1).astype(BF)

    def some_outputs(i, carry):
        cols = pl.ds(pl.multiple_of(i * step, step), step)
        out[:, cols] = dot(hidden_0, down_0[:, cols]) + dot(hidden_1, down_1[:, cols])
        return carry

    lax.fori_loop(0, 8, some_outputs, 0)


def expert_part(rows, mine, theirs):
    features, units = mine[0].shape
    count = rows.shape[0]
    vmem = pl.BlockSpec(memory_space=pltpu.VMEM)
    return pl.pallas_call(
        expert_kernel,
        out_shape=jax.ShapeDtypeStruct(rows.shape, F32),
        in_specs=[vmem] * 7,
        out_specs=vmem,
        compiler_params=pltpu.CompilerParams(vmem_limit_bytes=12 * 2**20),
        cost_estimate=pl.CostEstimate(
            flops=12 * count * features * units,
            bytes_accessed=12 * features * units,
            transcendentals=2 * count * units,
        ),
        name="expert",
    )(rows, *mine, *theirs)


def logits_kernel(*refs, sizes):
    count = len(sizes)
    pieces, wanted, head = refs[:count], refs[count], refs[count + 1]
    out, stacked, logits = refs[count + 2 :]
    at = 0
    for piece, size in zip(pieces, sizes):
        stacked[at : at + size, :] = piece[...]
        at += size
    half = head.shape[1] // 2
    for cols in (slice(0, half), slice(half, 2 * half)):
        logits[:, cols] = dot(stacked[...], head[:, cols])
    step = 64

    def some_rows(i, carry):
        here = pl.ds(pl.multiple_of(i * step, step), step)
        values = logits[here, :]
        peak = jnp.max(values, axis=1, keepdims=True)
        mass = jnp.sum(jnp.exp(values - peak), axis=1, keepdims=True)
        lane = lax.broadcasted_iota(I32, values.shape, 1)
        hit = jnp.sum(jnp.where(lane == wanted[here, :], values, 0.0), axis=1, keepdims=True)
        slot = lax.broadcasted_iota(I32, (step, 128), 1)
        out[here, :] = jnp.where(slot == 0, peak + jnp.log(mass), hit)
        return carry

    lax.fori_loop(0, at // step, some_rows, 0)


def logits_part(pieces, wanted, head):
    sizes = [piece.shape[0] for piece in pieces]
    count = sum(sizes)
    features, entries = head.shape
    vmem = pl.BlockSpec(memory_space=pltpu.VMEM)
    return pl.pallas_call(
        lambda *refs: logits_kernel(*refs, sizes=sizes),
        out_shape=jax.ShapeDtypeStruct((count, 128), F32),
        in_specs=[vmem] * (len(pieces) + 2),
        out_specs=vmem,
        scratch_shapes=[pltpu.VMEM((count, features), BF), pltpu.VMEM((count, entries), F32)],
        compiler_params=pltpu.CompilerParams(vmem_limit_bytes=10 * 2**20),
        cost_estimate=pl.CostEstimate(
            flops=2 * count * features * entries,
            bytes_accessed=2 * features * entries,
            transcendentals=count * entries,
        ),
        name="logits",
    )(*pieces, wanted.reshape(count, 1), head)


def on_device(
    rollout_states,
    lengths,
    group_ids,
    route_ids,
    route_weights,
    gain_in,
    w_gate,
    w_up,
    w_down,
    gain_out,
    head_weight,
    targets,
    policy_logp,
):
    own_x, own_z, own_y, own_c = (lax.axis_index(a) for a in ("dp", "z", "y", "c"))
    rows, pos_count, features = rollout_states.shape[1:]
    tokens = rows * pos_count
    wide = pos_count * features
    facts = jnp.pad(jnp.stack([group_ids, lengths], axis=1).astype(BF), ((0, 0), (0, 126)))
    block = jnp.concatenate([rollout_states.reshape(rows, wide), facts], axis=1)
    blocks = [block, shift(block, "dp", 1), shift(block, "dp", 2), shift(block, "dp", -1)]
    every = jnp.concatenate(blocks, axis=0)
    every, w_gate, w_up, w_down = lax.optimization_barrier((every, w_gate, w_up, w_down))
    local = jnp.arange(rows, dtype=I32)
    ids = jnp.concatenate([((own_x - k) % NX) * rows + local for k in range(NX)])
    owner = every[:, wide].astype(I32) % NX
    before = (owner[None, :] == owner[:, None]) & (ids[None, :] < ids[:, None])
    rank = jnp.sum(before.astype(I32), axis=1)
    place = jnp.where(owner == own_x, rank, rows)
    pick = (place[None, :] == local[:, None]).astype(BF)
    owned = dot(pick, every)
    owned_lengths = owned[:, wide + 1].astype(I32)
    states_wide = owned[:, :wide].reshape(tokens, features)
    mine = (w_gate[0], w_up[0], w_down[0])
    theirs = []
    for part in mine:
        theirs.append(pair_swap(part, 0))
    normed_in = scaled_norm(states_wide, gain_in).astype(BF)
    target = targets.reshape(tokens, 1)
    expert_ids = route_ids.reshape(tokens, -1)
    topk = expert_ids.shape[1]
    info = [expert_ids.astype(F32)]
    info += three_parts(policy_logp.reshape(tokens, 1))
    info += [(target // 256).astype(F32), (target % 256).astype(F32)]
    info = jnp.concatenate(info, axis=1)
    info = jnp.pad(info, ((0, 0), (0, 128 - info.shape[1]))).astype(BF)
    own = jnp.concatenate([normed_in, info], axis=1)
    every_z = sent_to_all(own, "z")
    halves = []
    for index in range(2):
        blocks = NZ // 2
        rows_in = every_z[index * blocks : (index + 1) * blocks].reshape(blocks * tokens, -1)
        count = rows_in.shape[0]
        ids = plain(rows_in[:, features:]).astype(F32)[:, :topk].astype(I32) - own_z * PLANE
        member = jnp.any(ids[:, :, None] == jnp.arange(PLANE, dtype=I32), axis=1)
        t = np.arange(count)
        earlier = (t[:, None] // tokens == t[None, :] // tokens) & (t[None, :] < t[:, None])
        rank = dot(jnp.asarray(earlier, BF), member.astype(BF)).astype(I32)
        slot = jnp.where(member, rank + jnp.asarray(t[:, None] // tokens * SLOT, I32), -1)
        spots = blocks * SLOT
        at = jnp.arange(spots, dtype=I32)
        spread = (slot.T[:, None, :] == at[None, :, None]).reshape(PLANE * spots, count)
        sender = dot(spread.astype(BF), rows_in[:, :features]).astype(BF)
        arrived = lax.all_to_all(
            sender.reshape(PLANE, spots, features), ("y", "c"), 0, 0, tiled=True
        ).reshape(-1, features)
        paired_rows = pair_swap(arrived, 1)
        halves.append((arrived, paired_rows))
    facts = plain(every_z[:, :, features:]).astype(F32)
    policy = facts[:, :, topk] + facts[:, :, topk + 1] + facts[:, :, topk + 2]
    column = jnp.stack([facts[:, :, topk + 3] * 256 + facts[:, :, topk + 4], policy])
    column = column.reshape(2, NZ * tokens)
    from_pair, own_part = [], []
    for index, (own, paired_rows) in enumerate(halves):
        for_pair = expert_part(paired_rows, mine, theirs)
        for_pair, own, column = lax.optimization_barrier((for_pair, own, column))
        from_pair.append(pair_swap(for_pair, 1))
        own_part.append(expert_part(own, mine, theirs))
        if index == 0:
            plane = sent_to_all(column, ("y", "c")).reshape(NY, NC, 2, NZ, tokens)
    all_targets = plane[:, :, 0].astype(I32).transpose(2, 0, 1, 3)
    all_policy = plane[:, :, 1].transpose(2, 0, 1, 3)
    blocks = NZ // 2
    order = np.arange(NZ * PLANE * SLOT).reshape(2, PLANE, blocks, SLOT)
    order = order.transpose(0, 2, 1, 3).reshape(-1)
    sort = order[:, None] == np.arange(len(order))[None, :]
    worked = []
    for own, peer in zip(own_part, from_pair):
        if worked:
            own, peer, *_ = lax.optimization_barrier((own, peer, worked[0]))
        else:
            own, all_targets, all_policy = lax.optimization_barrier((own, all_targets, all_policy))
        worked.append((own + peer).astype(BF))
    cut = len(order) // 2
    sort = jnp.asarray(sort, BF)
    home = (dot(sort[:, :cut], worked[0]) + dot(sort[:, cut:], worked[1])).astype(BF)
    returned = lax.all_to_all(
        home.reshape(-1, SLOT, features), EXPERT, 0, 0, tiled=True
    ).reshape(-1, features)
    gates = route_weights.reshape(tokens, -1)
    named = expert_ids[:, :, None] == jnp.arange(NZ * PLANE, dtype=I32)
    member = jnp.any(named, axis=1)
    weight = jnp.sum(jnp.where(named, gates[:, :, None], 0.0), axis=1)
    t = np.arange(tokens)
    rank = dot(jnp.asarray(t[None, :] < t[:, None], BF), member.astype(BF)).astype(I32)
    holds = member[:, :, None] & (rank[:, :, None] == jnp.arange(SLOT, dtype=I32))
    held = jnp.where(holds, weight[:, :, None], 0.0).reshape(tokens, -1)
    share = dot(jnp.concatenate(three_parts(held), axis=0).astype(BF), returned)
    share = share.reshape(3, tokens, features)
    routed = share[0] + share[1] + share[2]
    mixed_sum = states_wide + routed
    final_rows = scaled_norm(mixed_sum, gain_out).astype(BF)
    right = shift(final_rows, "y", 1)
    left = shift(final_rows, "y", -1)
    far = shift(right, "y", 1)
    col = jnp.concatenate([final_rows, right, far, left], axis=0)
    chunks = [([0], [col])]
    u, d = col, col
    for k in range(1, 4):
        u, d = shift(u, "z", 1), shift(d, "z", -1)
        chunks.append(([k, NZ - k], [u, d]))
    half = u.shape[0] // 2
    chunks.append(([4], [shift(u[:half], "z", 1), shift(d[half:], "z", -1)]))
    vocab_part = head_weight.shape[1]
    own_expert = (own_z * NY + own_y) * NC + own_c
    vocab_start = own_expert * vocab_part
    by_place = turned(all_targets, own_z, NZ)
    by_place = turned(by_place.transpose(1, 0, 2, 3), own_y, NY)
    by_place = turned(by_place.transpose(2, 1, 0, 3), own_c, NC)
    found = {}
    for dzs, pieces in chunks:
        other = [shift(piece, "c", 1) for piece in pieces]
        wanted = jnp.stack([by_place[dc, dz] for dc in range(NC) for dz in dzs]).reshape(-1)
        two = logits_part(pieces + other, wanted - vocab_start, head_weight)[:, :2]
        two = two.T.reshape(2, NC, len(dzs), NY, tokens)
        for i, dz in enumerate(dzs):
            found[dz] = two[:, :, i]
    stats = jnp.stack([found[dz] for dz in range(NZ)], axis=2)
    stats = turned(stats.transpose(2, 3, 1, 0, 4), own_z, NZ)
    stats = turned(stats.transpose(1, 0, 2, 3, 4), own_y, NY)
    stats = turned(stats.transpose(2, 1, 0, 3, 4), own_c, NC)
    stats = stats.transpose(3, 1, 2, 0, 4).reshape(2, -1)
    many = sent_to_all(stats, EXPERT)
    peak = jnp.max(many[:, 0], axis=0)
    mass = jnp.sum(jnp.exp(many[:, 0] - peak[None]), axis=0)
    ref_logp = jnp.sum(many[:, 1], axis=0) - (peak + jnp.log(mass))
    log_ratio = jnp.clip(ref_logp - all_policy.reshape(-1), -10.0, 10.0)
    token_value = (jnp.exp(log_ratio) - log_ratio - 1.0).reshape(-1, rows, pos_count)
    at = jnp.arange(NZ * PLANE, dtype=I32)
    position = at[:, None] * pos_count + jnp.arange(pos_count, dtype=I32)[None, :]
    inside = position[:, None, :] < owned_lengths[None, :, None]
    all_kl = jnp.where(inside, token_value, 0.0)
    token_kl = jnp.sum(jnp.where((at == own_expert)[:, None, None], all_kl, 0.0), axis=0)
    row_kl = jnp.sum(all_kl, axis=(0, 2)) / owned_lengths.astype(F32)
    return (token_kl.reshape(1, rows, pos_count), row_kl)


def solution(mesh):
    cut = Mesh(mesh.devices.reshape(NX, NZ, NY, NC), ("dp", *EXPERT))
    in_specs = (
        P(EXPERT, "dp", None, None),
        P("dp"),
        P("dp"),
        P(EXPERT, "dp", None, None),
        P(EXPERT, "dp", None, None),
        P(),
        P(EXPERT, None, "dp"),
        P(EXPERT, None, "dp"),
        P(EXPERT, "dp", None),
        P(),
        P(None, EXPERT),
        P(EXPERT, "dp", None),
        P(EXPERT, "dp", None),
    )
    out_specs = (P(EXPERT, "dp", None), P("dp"))
    return jax.shard_map(on_device, mesh=cut, in_specs=in_specs, out_specs=out_specs, check_vma=False)
```

```python
import jax
import jax.numpy as jnp
import numpy as np
from jax import lax
from jax.experimental import pallas as pl
from jax.experimental.layout import Layout, with_layout_constraint
from jax.experimental.pallas import tpu as pltpu
from jax.sharding import Mesh
from jax.sharding import PartitionSpec as P

BF = jnp.bfloat16
F32 = jnp.float32
I32 = jnp.int32
NX, NZ, NY, NC = 4, 8, 4, 2
PLANE = NY * NC
SLOT = 4
EXPERT = ("z", "y", "c")


def shift(value, axis, by):
    size = {"dp": NX, "z": NZ, "y": NY, "c": NC}[axis]
    return lax.ppermute(value, axis, [(i, (i + by) % size) for i in range(size)])


def pair_swap(value, parity):
    perm = []
    for x in range(NX):
        for e in range(NZ * NY * NC):
            if (e % NC + parity) % 2 == 0:
                peer = x ^ 1
            else:
                peer = (x + 1) % NX if x % 2 else (x - 1) % NX
            perm.append((x * NZ * PLANE + e, peer * NZ * PLANE + e))
    return lax.ppermute(value, ("dp", *EXPERT), perm)


def sent_to_all(value, axis):
    copies = jnp.broadcast_to(value, (lax.axis_size(axis), *value.shape))
    return lax.all_to_all(copies, axis, split_axis=0, concat_axis=0, tiled=True)


def turned(value, own, size):
    at = jnp.arange(size, dtype=I32)
    one = (own - at[:, None]) % size == at[None, :]
    one = one.reshape(size, size, *([1] * (value.ndim - 1)))
    return jnp.sum(jnp.where(one, value[None], jnp.zeros((), value.dtype)), axis=1)


def scaled_norm(values, gain_vec):
    mean_square = jnp.mean(values * values, axis=-1, keepdims=True)
    return values * lax.rsqrt(mean_square + 1e-06) * gain_vec


def plain(value):
    return with_layout_constraint(value, Layout(tuple(range(value.ndim))))


def dot(a, b):
    return jnp.dot(a, b, preferred_element_type=F32)


def three_parts(value):
    parts = []
    for _ in range(3):
        part = lax.reduce_precision(value, 8, 7)
        parts.append(part)
        value = value - part
    return parts


def expert_kernel(rows, gate_0, up_0, down_0, gate_1, up_1, down_1, out):
    count, features = rows.shape
    units = gate_0.shape[1]
    step = features // 8

    def some_features(i, sums):
        here = pl.ds(pl.multiple_of(i * step, step), step)
        given = rows[:, here]
        parts = [dot(given, ref[here, :]) for ref in (gate_0, up_0, gate_1, up_1)]
        return tuple(s + p for s, p in zip(sums, parts))

    zero = jnp.zeros((count, units), F32)
    gated_0, upped_0, gated_1, upped_1 = lax.fori_loop(0, 8, some_features, (zero,) * 4)
    hidden_0 = (gated_0 * jax.nn.sigmoid(gated_0) * upped_0).astype(BF)
    hidden_1 = (gated_1 * jax.nn.sigmoid(gated_1) * upped_1).astype(BF)

    def some_outputs(i, carry):
        cols = pl.ds(pl.multiple_of(i * step, step), step)
        out[:, cols] = dot(hidden_0, down_0[:, cols]) + dot(hidden_1, down_1[:, cols])
        return carry

    lax.fori_loop(0, 8, some_outputs, 0)


def expert_part(rows, mine, theirs):
    features, units = mine[0].shape
    count = rows.shape[0]
    vmem = pl.BlockSpec(memory_space=pltpu.VMEM)
    return pl.pallas_call(
        expert_kernel,
        out_shape=jax.ShapeDtypeStruct(rows.shape, F32),
        in_specs=[vmem] * 7,
        out_specs=vmem,
        compiler_params=pltpu.CompilerParams(vmem_limit_bytes=12 * 2**20),
        cost_estimate=pl.CostEstimate(
            flops=12 * count * features * units,
            bytes_accessed=12 * features * units,
            transcendentals=2 * count * units,
        ),
        name="expert",
    )(rows, *mine, *theirs)


def logits_kernel(*refs, sizes):
    count = len(sizes)
    pieces, wanted, head = refs[:count], refs[count], refs[count + 1]
    out, stacked, logits = refs[count + 2 :]
    at = 0
    for piece, size in zip(pieces, sizes):
        stacked[at : at + size, :] = piece[...]
        at += size
    half = head.shape[1] // 2
    for cols in (slice(0, half), slice(half, 2 * half)):
        logits[:, cols] = dot(stacked[...], head[:, cols])
    step = 64

    def some_rows(i, carry):
        here = pl.ds(pl.multiple_of(i * step, step), step)
        values = logits[here, :]
        peak = jnp.max(values, axis=1, keepdims=True)
        mass = jnp.sum(jnp.exp(values - peak), axis=1, keepdims=True)
        lane = lax.broadcasted_iota(I32, values.shape, 1)
        hit = jnp.sum(jnp.where(lane == wanted[here, :], values, 0.0), axis=1, keepdims=True)
        slot = lax.broadcasted_iota(I32, (step, 128), 1)
        out[here, :] = jnp.where(slot == 0, peak + jnp.log(mass), hit)
        return carry

    lax.fori_loop(0, at // step, some_rows, 0)


def logits_part(pieces, wanted, head):
    sizes = [piece.shape[0] for piece in pieces]
    count = sum(sizes)
    features, entries = head.shape
    vmem = pl.BlockSpec(memory_space=pltpu.VMEM)
    return pl.pallas_call(
        lambda *refs: logits_kernel(*refs, sizes=sizes),
        out_shape=jax.ShapeDtypeStruct((count, 128), F32),
        in_specs=[vmem] * (len(pieces) + 2),
        out_specs=vmem,
        scratch_shapes=[pltpu.VMEM((count, features), BF), pltpu.VMEM((count, entries), F32)],
        compiler_params=pltpu.CompilerParams(vmem_limit_bytes=10 * 2**20),
        cost_estimate=pl.CostEstimate(
            flops=2 * count * features * entries,
            bytes_accessed=2 * features * entries,
            transcendentals=count * entries,
        ),
        name="logits",
    )(*pieces, wanted.reshape(count, 1), head)


def on_device(
    rollout_states,
    lengths,
    group_ids,
    route_ids,
    route_weights,
    gain_in,
    w_gate,
    w_up,
    w_down,
    gain_out,
    head_weight,
    targets,
    policy_logp,
):
    own_x, own_z, own_y, own_c = (lax.axis_index(a) for a in ("dp", "z", "y", "c"))
    rows, pos_count, features = rollout_states.shape[1:]
    tokens = rows * pos_count
    wide = pos_count * features
    facts = jnp.pad(jnp.stack([group_ids, lengths], axis=1).astype(BF), ((0, 0), (0, 126)))
    block = jnp.concatenate([rollout_states.reshape(rows, wide), facts], axis=1)
    blocks = [block, shift(block, "dp", 1), shift(block, "dp", 2), shift(block, "dp", -1)]
    every = jnp.concatenate(blocks, axis=0)
    every, w_gate, w_up, w_down = lax.optimization_barrier((every, w_gate, w_up, w_down))
    local = jnp.arange(rows, dtype=I32)
    ids = jnp.concatenate([((own_x - k) % NX) * rows + local for k in range(NX)])
    owner = every[:, wide].astype(I32) % NX
    before = (owner[None, :] == owner[:, None]) & (ids[None, :] < ids[:, None])
    rank = jnp.sum(before.astype(I32), axis=1)
    place = jnp.where(owner == own_x, rank, rows)
    pick = (place[None, :] == local[:, None]).astype(BF)
    owned = dot(pick, every)
    owned_lengths = owned[:, wide + 1].astype(I32)
    states_wide = owned[:, :wide].reshape(tokens, features)
    mine = (w_gate[0], w_up[0], w_down[0])
    theirs = []
    for part in mine:
        theirs.append(pair_swap(part, 0))
    normed_in = scaled_norm(states_wide, gain_in).astype(BF)
    target = targets.reshape(tokens, 1)
    expert_ids = route_ids.reshape(tokens, -1)
    topk = expert_ids.shape[1]
    info = [expert_ids.astype(F32)]
    info += three_parts(policy_logp.reshape(tokens, 1))
    info += [(target // 256).astype(F32), (target % 256).astype(F32)]
    info = jnp.concatenate(info, axis=1)
    info = jnp.pad(info, ((0, 0), (0, 128 - info.shape[1]))).astype(BF)
    own = jnp.concatenate([normed_in, info], axis=1)
    up, down = [own], [own]
    for step in range(4):
        up.append(shift(up[-1], "z", 1))
        if step < 3:
            down.append(shift(down[-1], "z", -1))
    ring = up + down[:0:-1]
    rows_in = jnp.concatenate(ring, axis=0)
    count = rows_in.shape[0]
    ids = plain(rows_in[:, features:]).astype(F32)
    facts = ids.reshape(NZ, tokens, -1)
    ids = ids[:, :topk].astype(I32) - own_z * PLANE
    member = jnp.any(ids[:, :, None] == jnp.arange(PLANE, dtype=I32), axis=1)
    t = np.arange(count)
    earlier = (t[:, None] // tokens == t[None, :] // tokens) & (t[None, :] < t[:, None])
    rank = dot(jnp.asarray(earlier, BF), member.astype(BF)).astype(I32)
    from_z = (own_z - jnp.asarray(t // tokens, I32)) % NZ
    slot = jnp.where(member, rank + from_z[:, None] * SLOT, -1).T
    halves = []
    for index in range(2):
        spots = NZ // 2 * SLOT
        at = jnp.arange(spots, dtype=I32) + index * spots
        spread = (slot[:, None, :] == at[None, :, None]).reshape(PLANE * spots, count)
        sender = dot(spread.astype(BF), rows_in[:, :features]).astype(BF)
        arrived = lax.all_to_all(
            sender.reshape(PLANE, spots, features), ("y", "c"), 0, 0, tiled=True
        ).reshape(-1, features)
        paired_rows = pair_swap(arrived, 1)
        halves.append((arrived, paired_rows))
    policy = facts[:, :, topk] + facts[:, :, topk + 1] + facts[:, :, topk + 2]
    column = jnp.stack([facts[:, :, topk + 3] * 256 + facts[:, :, topk + 4], policy])
    column = turned(column.transpose(1, 0, 2), own_z, NZ).transpose(1, 0, 2)
    column = column.reshape(2, NZ * tokens)
    from_pair, own_part = [], []
    for index, (own, paired_rows) in enumerate(halves):
        for_pair = expert_part(paired_rows, mine, theirs)
        for_pair, own, column = lax.optimization_barrier((for_pair, own, column))
        from_pair.append(pair_swap(for_pair, 1))
        own_part.append(expert_part(own, mine, theirs))
        if index == 0:
            plane = sent_to_all(column, ("y", "c")).reshape(NY, NC, 2, NZ, tokens)
    all_targets = plane[:, :, 0].astype(I32).transpose(2, 0, 1, 3)
    all_policy = plane[:, :, 1].transpose(2, 0, 1, 3)
    blocks = NZ // 2
    order = np.arange(NZ * PLANE * SLOT).reshape(2, PLANE, blocks, SLOT)
    order = order.transpose(0, 2, 1, 3).reshape(-1)
    sort = order[:, None] == np.arange(len(order))[None, :]
    worked = []
    for own, peer in zip(own_part, from_pair):
        if worked:
            own, peer, *_ = lax.optimization_barrier((own, peer, worked[0]))
        else:
            own, all_targets, all_policy = lax.optimization_barrier((own, all_targets, all_policy))
        worked.append((own + peer).astype(BF))
    cut = len(order) // 2
    sort = jnp.asarray(sort, BF)
    home = (dot(sort[:, :cut], worked[0]) + dot(sort[:, cut:], worked[1])).astype(BF)
    returned = lax.all_to_all(
        home.reshape(-1, SLOT, features), EXPERT, 0, 0, tiled=True
    ).reshape(-1, features)
    gates = route_weights.reshape(tokens, -1)
    named = expert_ids[:, :, None] == jnp.arange(NZ * PLANE, dtype=I32)
    member = jnp.any(named, axis=1)
    weight = jnp.sum(jnp.where(named, gates[:, :, None], 0.0), axis=1)
    t = np.arange(tokens)
    rank = dot(jnp.asarray(t[None, :] < t[:, None], BF), member.astype(BF)).astype(I32)
    holds = member[:, :, None] & (rank[:, :, None] == jnp.arange(SLOT, dtype=I32))
    held = jnp.where(holds, weight[:, :, None], 0.0).reshape(tokens, -1)
    share = dot(jnp.concatenate(three_parts(held), axis=0).astype(BF), returned)
    share = share.reshape(3, tokens, features)
    routed = share[0] + share[1] + share[2]
    mixed_sum = states_wide + routed
    final_rows = scaled_norm(mixed_sum, gain_out).astype(BF)
    right = shift(final_rows, "y", 1)
    left = shift(final_rows, "y", -1)
    far = shift(right, "y", 1)
    col = jnp.concatenate([final_rows, right, far, left], axis=0)
    chunks = [([0], [col])]
    u, d = col, col
    for k in range(1, 4):
        u, d = shift(u, "z", 1), shift(d, "z", -1)
        chunks.append(([k, NZ - k], [u, d]))
    half = u.shape[0] // 2
    chunks.append(([4], [shift(u[:half], "z", 1), shift(d[half:], "z", -1)]))
    vocab_part = head_weight.shape[1]
    own_expert = (own_z * NY + own_y) * NC + own_c
    vocab_start = own_expert * vocab_part
    by_place = turned(all_targets, own_z, NZ)
    by_place = turned(by_place.transpose(1, 0, 2, 3), own_y, NY)
    by_place = turned(by_place.transpose(2, 1, 0, 3), own_c, NC)
    found = {}
    for dzs, pieces in chunks:
        other = [shift(piece, "c", 1) for piece in pieces]
        wanted = jnp.stack([by_place[dc, dz] for dc in range(NC) for dz in dzs]).reshape(-1)
        two = logits_part(pieces + other, wanted - vocab_start, head_weight)[:, :2]
        two = two.T.reshape(2, NC, len(dzs), NY, tokens)
        for i, dz in enumerate(dzs):
            found[dz] = two[:, :, i]
    stats = jnp.stack([found[dz] for dz in range(NZ)], axis=2)
    stats = turned(stats.transpose(2, 3, 1, 0, 4), own_z, NZ)
    stats = turned(stats.transpose(1, 0, 2, 3, 4), own_y, NY)
    stats = turned(stats.transpose(2, 1, 0, 3, 4), own_c, NC)
    stats = stats.transpose(3, 1, 2, 0, 4).reshape(2, -1)
    many = sent_to_all(stats, EXPERT)
    peak = jnp.max(many[:, 0], axis=0)
    mass = jnp.sum(jnp.exp(many[:, 0] - peak[None]), axis=0)
    ref_logp = jnp.sum(many[:, 1], axis=0) - (peak + jnp.log(mass))
    log_ratio = jnp.clip(ref_logp - all_policy.reshape(-1), -10.0, 10.0)
    token_value = (jnp.exp(log_ratio) - log_ratio - 1.0).reshape(-1, rows, pos_count)
    at = jnp.arange(NZ * PLANE, dtype=I32)
    position = at[:, None] * pos_count + jnp.arange(pos_count, dtype=I32)[None, :]
    inside = position[:, None, :] < owned_lengths[None, :, None]
    all_kl = jnp.where(inside, token_value, 0.0)
    token_kl = jnp.sum(jnp.where((at == own_expert)[:, None, None], all_kl, 0.0), axis=0)
    row_kl = jnp.sum(all_kl, axis=(0, 2)) / owned_lengths.astype(F32)
    return (token_kl.reshape(1, rows, pos_count), row_kl)


def solution(mesh):
    cut = Mesh(mesh.devices.reshape(NX, NZ, NY, NC), ("dp", *EXPERT))
    in_specs = (
        P(EXPERT, "dp", None, None),
        P("dp"),
        P("dp"),
        P(EXPERT, "dp", None, None),
        P(EXPERT, "dp", None, None),
        P(),
        P(EXPERT, None, "dp"),
        P(EXPERT, None, "dp"),
        P(EXPERT, "dp", None),
        P(),
        P(None, EXPERT),
        P(EXPERT, "dp", None),
        P(EXPERT, "dp", None),
    )
    out_specs = (P(EXPERT, "dp", None), P("dp"))
    return jax.shard_map(on_device, mesh=cut, in_specs=in_specs, out_specs=out_specs, check_vma=False)
```
